32 devices in a mesh: ey: 4 (over z), ex: 8 (over y, x, core).
Axes of the slice: x: 2, y: 2, z: 4, core: 2. Of those that a mesh axis runs over, the one named last changes fastest.
Arguments:
- x: bfloat16 [512, 2048], P(('ey', 'ex'))
- kv_k: bfloat16 [512, 256, 4, 128], P(('ey', 'ex'))
- kv_v: bfloat16 [512, 256, 4, 128], P(('ey', 'ex'))
- lens: int32 [512], P(('ey', 'ex'))
- topk_idx: int32 [512, 4], P(('ey', 'ex'))
- gates: float32 [512, 4], P(('ey', 'ex'))
- ln1: bfloat16 [2048], replicated
- wq: bfloat16 [2048, 4096], replicated
- wo: bfloat16 [4096, 2048], replicated
- ln2: bfloat16 [2048], replicated
- ws1: bfloat16 [2048, 5632], replicated
- ws3: bfloat16 [2048, 5632], replicated
- ws2: bfloat16 [5632, 2048], replicated
- w1: bfloat16 [64, 2048, 1408], P(('ey', 'ex'))
- w3: bfloat16 [64, 2048, 1408], P(('ey', 'ex'))
- w2: bfloat16 [64, 1408, 2048], P(('ey', 'ex'))
Outputs:
- output: bfloat16 [512, 2048], P(('ey', 'ex'))
All inputs are finite; a program needn't handle non-finite values.
Results may differ from the reference program's by a relative error of at most 0.0124602.
Values are sent between devices in bfloat16 or wider.
A program may use at most 1 GiB of HBM per device.

```python
import jax
import jax.numpy as jnp
from jax import lax

DEVICES = 32
B_DEV = 16
L = 256
D = 2048
HEADS = 32
KV_HEADS = 4
HEAD = 128
F = 1408
FS = 5632
E = 64
TOP = 4
EPS = 1e-6
B = DEVICES * B_DEV
E_DEV = E // DEVICES
CAP = B_DEV - B_DEV // 8
GROUP = HEADS // KV_HEADS


def _normal(key, shape, scale):
    return (scale * jax.random.normal(key, shape, jnp.float32)).astype(jnp.bfloat16)


def _route_ids(key):
    expert_ids = jnp.arange(E)
    cold_dev = (expert_ids >= 2 * E_DEV) & (expert_ids < 3 * E_DEV)
    weight = jnp.where(expert_ids >= E - 2, 1, jnp.where(cold_dev, E * 37 // 5, E)).astype(jnp.uint32)
    arrival = (jax.random.bits(key, (B, E), jnp.uint32) >> 12) * weight[None, :]
    return jnp.argsort(arrival, axis=-1)[:, :TOP].astype(jnp.int32)


def setup_inputs(seed: int = 0) -> dict:
    ks = jax.random.split(jax.random.PRNGKey(seed), 16)
    dk = jax.random.split(jax.random.fold_in(jax.random.PRNGKey(seed), 7), 3)
    dev = jnp.arange(B) // B_DEV
    far = (dev % 4) == 0
    far_len = jax.random.randint(dk[0], (B,), 3 * L // 4, L, jnp.int32)
    near_len = jax.random.randint(dk[1], (B,), 0, L // 16, jnp.int32)
    lens = jnp.clip(jnp.where(far, far_len, near_len), 1, L).astype(jnp.int32)
    topk_idx = _route_ids(dk[2])
    gates = 2.5 * jax.nn.softmax(0.5 * jax.random.normal(ks[5], (B, TOP), jnp.float32), axis=-1)
    return {
        "x": _normal(ks[0], (B, D), 1.0),
        "kv_k": _normal(ks[1], (B, L, KV_HEADS, HEAD), 2.0),
        "kv_v": _normal(ks[2], (B, L, KV_HEADS, HEAD), 1.0),
        "lens": lens,
        "topk_idx": topk_idx.astype(jnp.int32),
        "gates": gates,
        "ln1": (1.0 + 0.1 * jax.random.normal(ks[6], (D,), jnp.float32)).astype(jnp.bfloat16),
        "wq": _normal(ks[7], (D, HEADS * HEAD), D ** -0.5),
        "wo": _normal(ks[8], (HEADS * HEAD, D), (HEADS * HEAD) ** -0.5),
        "ln2": (1.0 + 0.1 * jax.random.normal(ks[9], (D,), jnp.float32)).astype(jnp.bfloat16),
        "ws1": _normal(ks[10], (D, FS), D ** -0.5),
        "ws3": _normal(ks[11], (D, FS), D ** -0.5),
        "ws2": _normal(ks[12], (FS, D), FS ** -0.5),
        "w1": _normal(ks[13], (E, D, F), D ** -0.5),
        "w3": _normal(ks[14], (E, D, F), D ** -0.5),
        "w2": _normal(ks[15], (E, F, D), F ** -0.5),
    }


def _rms(v, w):
    v32 = v.astype(jnp.float32)
    r = lax.rsqrt(jnp.mean(v32 * v32, axis=-1, keepdims=True) + EPS)
    return (v32 * r * w.astype(jnp.float32)).astype(jnp.bfloat16)


def _swiglu(a, w1, w3, w2):
    z1 = jnp.dot(a, w1, preferred_element_type=jnp.float32)
    z3 = jnp.dot(a, w3, preferred_element_type=jnp.float32)
    g = (jax.nn.silu(z1) * z3).astype(jnp.bfloat16)
    return jnp.dot(g, w2, preferred_element_type=jnp.float32)


def _attend(args):
    q, k, v, n = args
    s = jnp.einsum("kgh,lkh->kgl", q.astype(jnp.float32), k.astype(jnp.float32)) * HEAD ** -0.5
    s = jnp.where(jnp.arange(L) < n, s, -jnp.inf)
    p = jax.nn.softmax(s, axis=-1).astype(jnp.bfloat16)
    return jnp.einsum("kgl,lkh->kgh", p.astype(jnp.float32), v.astype(jnp.float32)).astype(jnp.bfloat16)


def reference(x, kv_k, kv_v, lens, topk_idx, gates, ln1, wq, wo, ln2, ws1, ws3, ws2, w1, w3, w2):
    a = _rms(x, ln1)
    q = jnp.dot(a, wq, preferred_element_type=jnp.float32).astype(jnp.bfloat16)
    o = lax.map(_attend, (q.reshape(B, KV_HEADS, GROUP, HEAD), kv_k, kv_v, lens))
    attn = jnp.dot(o.reshape(B, HEADS * HEAD), wo, preferred_element_type=jnp.float32)
    h = (x.astype(jnp.float32) + attn).astype(jnp.bfloat16)
    u = _rms(h, ln2)
    shared = _swiglu(u, ws1, ws3, ws2)
    blk = topk_idx.reshape(DEVICES, B_DEV * TOP)
    oh = jax.nn.one_hot(blk, E, dtype=jnp.int32)
    rank = jnp.sum((jnp.cumsum(oh, axis=1) - oh) * oh, axis=-1)
    src = jnp.arange(DEVICES)[:, None]
    slot = jnp.where(rank < CAP, (blk * DEVICES + src) * CAP + rank, E * DEVICES * CAP).reshape(-1)
    tok = jnp.arange(B * TOP) // TOP
    tok_buf = jnp.full((E * DEVICES * CAP,), B, jnp.int32).at[slot].set(tok, mode="drop")
    gate_buf = jnp.zeros((E * DEVICES * CAP,), jnp.float32).at[slot].set(gates.reshape(-1), mode="drop")

    def expert(acc, xs):
        t, g, e1, e3, e2 = xs
        rows = jnp.take(u, t, axis=0, mode="fill", fill_value=0)
        out = _swiglu(rows, e1, e3, e2).astype(jnp.bfloat16).astype(jnp.float32)
        return acc.at[t].add(g[:, None] * out, mode="drop"), None

    routed, _ = lax.scan(expert, jnp.zeros((B, D), jnp.float32),
                         (tok_buf.reshape(E, DEVICES * CAP), gate_buf.reshape(E, DEVICES * CAP), w1, w3, w2))
    return (h.astype(jnp.float32) + shared + routed).astype(jnp.bfloat16)
```

```python
import functools

import jax
import jax.numpy as jnp
from jax import lax
from jax.experimental import pallas as pl
from jax.experimental.pallas import tpu as pltpu
from jax.sharding import PartitionSpec as P

EPS = 1e-6
GRP = ("ey", "ex")
MESH = pl.DeviceIdType.MESH
BF16, F32 = jnp.bfloat16, jnp.float32

CHUNKS = ((0, 2), (2, 1), (3, 1))
SHARED_DEVS = 22


def _rms(v, w):
    v32 = v.astype(F32)
    r = lax.rsqrt(jnp.mean(v32 * v32, axis=-1, keepdims=True) + EPS)
    return (v32 * r * w.astype(F32)).astype(BF16)


def _attention_block(x, kv_k, kv_v, lens, ln1, wq, wo):
    b, d = x.shape
    _, l, kvh, hd = kv_k.shape
    nh = wq.shape[1] // hd
    a = _rms(x, ln1)
    q = jnp.dot(a, wq, preferred_element_type=F32).astype(BF16).reshape(b, kvh, nh // kvh, hd)
    s = jnp.einsum("bkgh,blkh->bkgl", q, kv_k, preferred_element_type=F32) * hd ** -0.5
    s = jnp.where(jnp.arange(l) < lens[:, None, None, None], s, -jnp.inf)
    p = jax.nn.softmax(s, axis=-1).astype(BF16)
    o = jnp.einsum("bkgl,blkh->bkgh", p, kv_v, preferred_element_type=F32).astype(BF16)
    attn = jnp.dot(o.reshape(b, nh * hd), wo, preferred_element_type=F32)
    return (x.astype(F32) + attn).astype(BF16)


def _moe_kernel(h_ref, ln_ref, idx_ref, gate_ref, s1_hbm, s3_hbm, s2_hbm, w1_hbm, w3_hbm, w2_hbm, y_ref,
                U, GW, GB, Pb, R1, R2x, R2y, R3x, R3y, R4, G, GS, W1, W3, W2, S1, S3, S2,
                wsem, ag_s, ag_r, gw_s, gw_r, rs_s, rs_r):
    z = lax.axis_index("ey")
    ex = lax.axis_index("ex")
    c = lax.rem(ex, 2)
    xx = lax.rem(lax.div(ex, 2), 2)
    yy = lax.div(ex, 4)
    dev = z * 8 + ex
    bdev, d = h_ref.shape
    f = W1.shape[2]
    cap = bdev - bdev // 8
    half = d // 2
    H0, H1 = pl.ds(0, half), pl.ds(half, half)
    ALL = pl.ds(0, d)
    core = (z, ex + 1 - 2 * c)
    xn = (z, ex + 2 - 4 * xx)
    yn = (z, ex + 4 - 8 * yy)
    zp = {1: (z + 1 - 2 * lax.rem(z, 2), ex), 2: (z + 2 - 4 * lax.div(z, 2), ex), 3: (3 - z, ex)}

    def rows(k, dc, dq, n=1):
        return pl.ds(((k * 2 + dc) * 4 + dq) * bdev, n * bdev)

    loads = {}

    def load(name, i, src, dst):
        cp = pltpu.make_async_copy(src, dst, wsem.at[i])
        cp.start()
        loads[name] = cp

    load("w1_0", 0, w1_hbm.at[0], W1.at[0])
    load("w3_0", 1, w3_hbm.at[0], W3.at[0])
    load("w1_1", 2, w1_hbm.at[1], W1.at[1])
    load("w3_1", 3, w3_hbm.at[1], W3.at[1])
    scol = pl.ds(pl.multiple_of(lax.rem(dev, SHARED_DEVS) * 256, 256), 256)
    load("s1", 6, s1_hbm.at[:, scol], S1)
    load("s3", 7, s3_hbm.at[:, scol], S3)
    load("s2", 8, s2_hbm.at[scol, :], S2)
    load("w2_0", 4, w2_hbm.at[0], W2.at[0])
    load("w2_1", 5, w2_hbm.at[1], W2.at[1])
    waited = set()

    def need(*names):
        for n in names:
            if n not in waited:
                waited.add(n)
                loads[n].wait()

    u = _rms(h_ref[...], ln_ref[...])
    U[rows(0, 0, 0), :] = u
    lane = lax.broadcasted_iota(jnp.int32, (bdev, 128), 1)
    oh = jnp.zeros((bdev, 128), F32)
    gm = jnp.zeros((bdev, 128), F32)
    for j in range(idx_ref.shape[1]):
        hit = idx_ref[:, j:j + 1] == lane
        oh = oh + jnp.where(hit, 1.0, 0.0)
        gm = gm + jnp.where(hit, gate_ref[:, j:j + 1], 0.0)
    r_i = lax.broadcasted_iota(jnp.int32, (bdev, bdev), 0)
    c_i = lax.broadcasted_iota(jnp.int32, (bdev, bdev), 1)
    tril = jnp.where(c_i < r_i, 1.0, 0.0)
    rank = jnp.dot(tril.astype(BF16), oh.astype(BF16), preferred_element_type=F32)
    GW[rows(0, 0, 0), :] = jnp.where(rank < cap - 0.5, gm, 0.0)

    barrier = pltpu.get_barrier_semaphore()
    for n in (core, xn, yn, zp[1], zp[2], zp[3]):
        pl.semaphore_signal(barrier, inc=1, device_id=n, device_id_type=MESH)
    pl.semaphore_wait(barrier, 6)

    def send(src, dst, ss, rs, to):
        cp = pltpu.make_async_remote_copy(src_ref=src, dst_ref=dst, send_sem=ss, recv_sem=rs,
                                          device_id=to, device_id_type=MESH)
        cp.start()
        return cp

    sent = []

    ag = {}

    def ag_send(key, i, src_rows, dst_rows, cols, to):
        cp = send(U.at[src_rows, cols], U.at[dst_rows, cols], ag_s.at[i], ag_r.at[i], to)
        ag[key] = cp
        sent.append(cp)

    gw = {}

    def gw_send(key, i, src_rows, dst_rows, to):
        cp = send(GW.at[src_rows, :], GW.at[dst_rows, :], gw_s.at[i], gw_r.at[i], to)
        gw[key] = cp
        sent.append(cp)

    def a2(k):
        ag_send(("2x", k), 3 + k * 6, rows(k, 0, 0), rows(k, 0, 1), H0, xn)
        ag_send(("2y", k), 4 + k * 6, rows(k, 0, 0), rows(k, 0, 2), H1, yn)
        gw_send(("2", k), 3 + k * 3, rows(k, 0, 0), rows(k, 0, 1), xn)

    def a3(k):
        ag[("2x", k)].wait_recv()
        ag_send(("3y", k), 5 + k * 6, rows(k, 0, 0, 2), rows(k, 0, 2, 2), H0, yn)
        ag[("2y", k)].wait_recv()
        ag_send(("3x", k), 6 + k * 6, rows(k, 0, 0), rows(k, 0, 1), H1, xn)
        ag_send(("3d", k), 7 + k * 6, rows(k, 0, 2), rows(k, 0, 3), H1, xn)
        gw[("2", k)].wait_recv()
        gw_send(("3", k), 4 + k * 3, rows(k, 0, 0, 2), rows(k, 0, 2, 2), yn)

    def a4(k):
        for n in ("3y", "3x", "3d"):
            ag[(n, k)].wait_recv()
        ag_send(("4", k), 8 + k * 6, rows(k, 0, 0, 4), rows(k, 1, 0, 4), ALL, core)
        gw[("3", k)].wait_recv()
        gw_send(("4", k), 5 + k * 3, rows(k, 0, 0, 4), rows(k, 1, 0, 4), core)

    def a5(k):
        ag[("4", k)].wait_recv()
        gw[("4", k)].wait_recv()

    def zwait(k):
        ag[("z", k)].wait_recv()
        gw[("z", k)].wait_recv()
        a2(k)

    for k in (1, 2, 3):
        ag_send(("z", k), k - 1, rows(0, 0, 0), rows(k, 0, 0), ALL, zp[k])
        gw_send(("z", k), k - 1, rows(0, 0, 0), rows(k, 0, 0), zp[k])
    a2(0)
    zwait(1)
    a3(0)
    zwait(2)
    a3(1)
    a4(0)
    zwait(3)
    a3(2)
    a4(1)
    a5(0)

    rs = {}

    def rs_send(key, i, src, dst, to):
        cp = send(src, dst, rs_s.at[i], rs_r.at[i], to)
        rs[key] = cp
        sent.append(cp)

    def s1(k):
        rs_send(("1", k), k * 8, Pb.at[rows(k, 1, 0, 4), :], R1.at[pl.ds(k * 64, 64), :], core)

    def s2(k):
        rs[("1", k)].wait_recv()
        Pb[rows(k, 0, 0, 4), :] = Pb[rows(k, 0, 0, 4), :] + R1[pl.ds(k * 64, 64), :]
        rs_send(("2y", k), k * 8 + 1, Pb.at[rows(k, 0, 2, 2), H0], R2y.at[pl.ds(k * 32, 32), :], yn)
        rs_send(("2x", k), k * 8 + 2, Pb.at[rows(k, 0, 1), H1], R2x.at[pl.ds(k * 32, 16), :], xn)
        rs_send(("2d", k), k * 8 + 3, Pb.at[rows(k, 0, 3), H1], R2x.at[pl.ds(k * 32 + 16, 16), :], xn)

    def s3(k):
        rs[("2y", k)].wait_recv()
        Pb[rows(k, 0, 0, 2), H0] = Pb[rows(k, 0, 0, 2), H0] + R2y[pl.ds(k * 32, 32), :]
        rs_send(("3x", k), k * 8 + 4, Pb.at[rows(k, 0, 1), H0], R3x.at[pl.ds(k * 16, 16), :], xn)
        rs[("2x", k)].wait_recv()
        rs[("2d", k)].wait_recv()
        Pb[rows(k, 0, 2), H1] = Pb[rows(k, 0, 2), H1] + R2x[pl.ds(k * 32 + 16, 16), :]
        rs_send(("3y", k), k * 8 + 5, Pb.at[rows(k, 0, 2), H1], R3y.at[pl.ds(k * 16, 16), :], yn)
        Pb[rows(k, 0, 0), H1] = Pb[rows(k, 0, 0), H1] + R2x[pl.ds(k * 32, 16), :]

    def s4(k):
        rs[("3x", k)].wait_recv()
        Pb[rows(k, 0, 0), H0] = Pb[rows(k, 0, 0), H0] + R3x[pl.ds(k * 16, 16), :]
        rs[("3y", k)].wait_recv()
        Pb[rows(k, 0, 0), H1] = Pb[rows(k, 0, 0), H1] + R3y[pl.ds(k * 16, 16), :]
        if k:
            rs_send(("4", k), k * 8 + 6, Pb.at[rows(k, 0, 0), :], R4.at[pl.ds(k * 16, 16), :], zp[k])

    def up(uval, wa, wb, gdst, tiles):
        def step(t, _):
            col = pl.ds(pl.multiple_of(t * 128, 128), 128)
            w = jnp.concatenate([wa[:, col], wb[:, col]], axis=1)
            zz = jnp.dot(uval[...], w, preferred_element_type=F32)
            z1, z3 = zz[:, :128], zz[:, 128:]
            gdst[:, col] = (z1 * jax.nn.sigmoid(z1) * z3).astype(BF16)
            return 0
        lax.fori_loop(0, tiles, step, 0)

    def chunk(k0, n, hooks):
        m = n * 8 * bdev
        cr = pl.ds(k0 * 8 * bdev, m)
        mr = pl.ds(0, m)
        uv = U.at[cr, :]
        lanes = lax.broadcasted_iota(jnp.int32, (m, 128), 1)
        for e in range(2):
            gv = jnp.sum(jnp.where(lanes == dev * 2 + e, GW[cr, :], 0.0), axis=1, keepdims=True)
            GB[e, mr, :] = jnp.broadcast_to(gv, (m, 128))
        for e in range(2):
            need(f"w1_{e}", f"w3_{e}")
            up(uv, W1.at[e], W3.at[e], G.at[e, mr, :], f // 128)
            hooks[e]()
        need("s1", "s3")

        @pl.when(dev < SHARED_DEVS)
        def _():
            up(uv, S1, S3, GS.at[mr, :], 2)

        @pl.when(dev >= SHARED_DEVS)
        def _():
            GS[mr, :] = jnp.zeros((m, 256), BF16)

        need("w2_0", "w2_1", "s2")

        def step(t, _):
            col = pl.ds(pl.multiple_of(t * 256, 256), 256)
            acc = jnp.dot(GS[mr, :], S2[:, col], preferred_element_type=F32)
            for e in range(2):
                r = jnp.dot(G[e, mr, :], W2[e, :, col], preferred_element_type=F32).astype(BF16).astype(F32)
                g = GB[e, mr, :]
                g = jnp.concatenate([g, g], axis=1)
                acc = acc + jnp.where(g > 0, g * r, 0.0)
            Pb[cr, col] = acc
            return 0
        lax.fori_loop(0, 4, step, 0)
        hooks[2]()
        lax.fori_loop(4, 8, step, 0)
        hooks[3]()

    def nop():
        pass

    a5(1)

    def h_a():
        a3(3)
        a4(2)

    def h_b():
        a5(2)
        a4(3)

    chunk(0, 2, (h_a, h_b, lambda: a5(3), lambda: (s1(0), s1(1))))
    chunk(2, 1, (lambda: (s2(0), s2(1)), lambda: (s3(0), s3(1)), lambda: (s4(0), s4(1)), lambda: s1(2)))
    chunk(3, 1, (lambda: s2(2), lambda: s3(2), lambda: s4(2), lambda: s1(3)))
    s2(3)
    s3(3)
    s4(3)

    acc = h_ref[...].astype(F32) + Pb[rows(0, 0, 0), :]
    for k in (1, 2, 3):
        rs[("4", k)].wait_recv()
        acc = acc + R4[pl.ds(k * 16, 16), :]
    y_ref[...] = acc.astype(BF16)
    for cp in sent:
        cp.wait_send()


def solution(mesh):
    def body(x, kv_k, kv_v, lens, idx, gates, ln1, wq, wo, ln2, ws1, ws3, ws2, w1, w3, w2):
        bdev, d = x.shape
        f = w1.shape[2]
        rows = bdev * 32
        h = _attention_block(x, kv_k, kv_v, lens, ln1, wq, wo)
        vm = pl.BlockSpec(memory_space=pltpu.VMEM)
        hbm = pl.BlockSpec(memory_space=pl.ANY)
        mmax = max(n for _, n in CHUNKS) * 8 * bdev
        return pl.pallas_call(
            _moe_kernel,
            out_shape=jax.ShapeDtypeStruct((bdev, d), BF16),
            in_specs=[vm] * 4 + [hbm] * 6,
            out_specs=vm,
            scratch_shapes=[
                pltpu.VMEM((rows, d), BF16),
                pltpu.VMEM((rows, 128), F32),
                pltpu.VMEM((2, mmax, 128), F32),
                pltpu.VMEM((rows, d), F32),
                pltpu.VMEM((rows // 2, d), F32),
                pltpu.VMEM((128, d // 2), F32),
                pltpu.VMEM((128, d // 2), F32),
                pltpu.VMEM((64, d // 2), F32),
                pltpu.VMEM((64, d // 2), F32),
                pltpu.VMEM((64, d), F32),
                pltpu.VMEM((2, mmax, f), BF16),
                pltpu.VMEM((mmax, 256), BF16),
                pltpu.VMEM((2, d, f), BF16),
                pltpu.VMEM((2, d, f), BF16),
                pltpu.VMEM((2, f, d), BF16),
                pltpu.VMEM((d, 256), BF16),
                pltpu.VMEM((d, 256), BF16),
                pltpu.VMEM((256, d), BF16),
                pltpu.SemaphoreType.DMA((9,)),
                pltpu.SemaphoreType.DMA((28,)),
                pltpu.SemaphoreType.DMA((28,)),
                pltpu.SemaphoreType.DMA((16,)),
                pltpu.SemaphoreType.DMA((16,)),
                pltpu.SemaphoreType.DMA((32,)),
                pltpu.SemaphoreType.DMA((32,)),
            ],
            compiler_params=pltpu.CompilerParams(
                collective_id=0, has_side_effects=True, vmem_limit_bytes=60 * 1024 * 1024
            ),
        )(h, ln2.reshape(1, d), idx, gates, ws1, ws3, ws2, w1, w3, w2)

    rows = P(GRP)
    rep = P()
    return jax.shard_map(
        body, mesh=mesh,
        in_specs=(rows, rows, rows, rows, rows, rows, rep, rep, rep, rep, rep, rep, rep, rows, rows, rows),
        out_specs=rows, check_vma=False)
```

```python
import functools

import jax
import jax.numpy as jnp
from jax import lax
from jax.experimental import pallas as pl
from jax.experimental.pallas import tpu as pltpu
from jax.sharding import PartitionSpec as P

EPS = 1e-6
GRP = ("ey", "ex")
MESH = pl.DeviceIdType.MESH
BF16, F32 = jnp.bfloat16, jnp.float32

SHARED_DEVS = 22
CHUNKS = ((1, 1), (2, 1), (3, 1), (0, 1))
UNROLL, UNROLL2 = 8, 4


def HOOKS(ci, a2, zwait, a3, a4, a5, s1, s2, s3, s4):
    order = [k for k, _ in CHUNKS]
    k = order[ci]
    ev = {i: [] for i in range(5)}
    if ci == 0:
        ev[0] += [(a3, 3), (a4, 2)]
        ev[1] += [(a4, 0)]
        ev[2] += [(a4, 3)]
    if ci >= 2:
        ev[1] += [(s4, order[ci - 2], 0), (s4, order[ci - 2], 1)]
    if ci >= 1:
        ev[0] += [(s2, order[ci - 1], 0), (s2, order[ci - 1], 1)]
    ev[3] += [(s1, k, 0)]
    ev[4] += [(s1, k, 1)]
    if ci >= 1:
        ev[4] += [(s3, order[ci - 1], 0), (s3, order[ci - 1], 1)]
    return ev


def _rms(v, w):
    v32 = v.astype(F32)
    r = lax.rsqrt(jnp.mean(v32 * v32, axis=-1, keepdims=True) + EPS)
    return (v32 * r * w.astype(F32)).astype(BF16)


def _attention_block(x, kv_k, kv_v, lens, ln1, wq, wo):
    b, d = x.shape
    _, l, kvh, hd = kv_k.shape
    nh = wq.shape[1] // hd
    a = _rms(x, ln1)
    q = jnp.dot(a, wq, preferred_element_type=F32).astype(BF16).reshape(b, kvh, nh // kvh, hd)
    s = jnp.einsum("bkgh,blkh->bkgl", q, kv_k, preferred_element_type=F32) * hd ** -0.5
    s = jnp.where(jnp.arange(l) < lens[:, None, None, None], s, -jnp.inf)
    p = jax.nn.softmax(s, axis=-1).astype(BF16)
    o = jnp.einsum("bkgl,blkh->bkgh", p, kv_v, preferred_element_type=F32).astype(BF16)
    attn = jnp.dot(o.reshape(b, nh * hd), wo, preferred_element_type=F32)
    return (x.astype(F32) + attn).astype(BF16)


def _moe_kernel(h_ref, ln_ref, idx_ref, gate_ref, s1_hbm, s3_hbm, s2_hbm, w1_hbm, w3_hbm, w2_hbm, y_ref,
                U, GW, GB, Pb, R1, R2x, R2y, R3x, R3y, R4, G, W13, W2, S2,
                wsem, w2sem, s2sem, ag_s, ag_r, gw_s, gw_r, rs_s, rs_r):
    z = lax.axis_index("ey")
    ex = lax.axis_index("ex")
    c = lax.rem(ex, 2)
    xx = lax.rem(lax.div(ex, 2), 2)
    yy = lax.div(ex, 4)
    dev = z * 8 + ex
    bdev, d = h_ref.shape
    f = w1_hbm.shape[2]
    cap = bdev - bdev // 8
    half = d // 2
    H0, H1 = pl.ds(0, half), pl.ds(half, half)
    ALL = pl.ds(0, d)
    core = (z, ex + 1 - 2 * c)
    xn = (z, ex + 2 - 4 * xx)
    yn = (z, ex + 4 - 8 * yy)
    zp = {1: (z + 1 - 2 * lax.rem(z, 2), ex), 2: (z + 2 - 4 * lax.div(z, 2), ex), 3: (3 - z, ex)}

    def rows(k, dc, dq, n=1):
        return pl.ds(((k * 2 + dc) * 4 + dq) * bdev, n * bdev)

    nt = f // 128
    L0, L1 = pl.ds(0, 128), pl.ds(128, 128)

    def load(src, dst, sem):
        pltpu.make_async_copy(src, dst, sem).start()

    def load13(a, b, e, base, count):
        def step(t, _):
            col = pl.ds(pl.multiple_of(t * 128, 128), 128)
            load(a.at[e, :, col], W13.at[base + t, :, L0], wsem.at[base + t])
            load(b.at[e, :, col], W13.at[base + t, :, L1], wsem.at[base + t])
            return 0
        lax.fori_loop(0, count, step, 0)

    load13(w1_hbm, w3_hbm, 0, 0, nt)
    load13(w1_hbm, w3_hbm, 1, nt, nt)
    sbase = lax.rem(dev, SHARED_DEVS) * 256
    for t in range(2):
        col = pl.ds(pl.multiple_of(sbase + t * 128, 128), 128)
        load(s1_hbm.at[:, col], W13.at[2 * nt + t, :, L0], wsem.at[2 * nt + t])
        load(s3_hbm.at[:, col], W13.at[2 * nt + t, :, L1], wsem.at[2 * nt + t])
    scol = pl.ds(pl.multiple_of(sbase, 256), 256)

    def load2(t, _):
        col = pl.ds(pl.multiple_of(t * 256, 256), 256)
        for e in range(2):
            load(w2_hbm.at[e, :, col], W2.at[t, e], w2sem.at[t])
        load(s2_hbm.at[scol, col], S2.at[t], s2sem.at[t])
        return 0
    lax.fori_loop(0, d // 256, load2, 0)

    def got(ref, sem):
        pltpu.make_async_copy(ref, ref, sem).wait()

    u = _rms(h_ref[...], ln_ref[...])
    U[rows(0, 0, 0), :] = u
    lane = lax.broadcasted_iota(jnp.int32, (bdev, 128), 1)
    oh = jnp.zeros((bdev, 128), F32)
    gm = jnp.zeros((bdev, 128), F32)
    for j in range(idx_ref.shape[1]):
        hit = idx_ref[:, j:j + 1] == lane
        oh = oh + jnp.where(hit, 1.0, 0.0)
        gm = gm + jnp.where(hit, gate_ref[:, j:j + 1], 0.0)
    r_i = lax.broadcasted_iota(jnp.int32, (bdev, bdev), 0)
    c_i = lax.broadcasted_iota(jnp.int32, (bdev, bdev), 1)
    tril = jnp.where(c_i < r_i, 1.0, 0.0)
    rank = jnp.dot(tril.astype(BF16), oh.astype(BF16), preferred_element_type=F32)
    GW[rows(0, 0, 0), :] = jnp.where(rank < cap - 0.5, gm, 0.0)

    SC0 = jax.named_scope
    barrier = pltpu.get_barrier_semaphore()
    for n in (core, xn, yn, zp[1], zp[2], zp[3]):
        pl.semaphore_signal(barrier, inc=1, device_id=n, device_id_type=MESH)
    with SC0("barrier"):
        pl.semaphore_wait(barrier, 6)

    class send:
        def __init__(self, *args):
            self.args = args
            self.make().start()

        def make(self):
            src, dst, ss, rs, to = self.args
            return pltpu.make_async_remote_copy(src_ref=src(), dst_ref=dst(), send_sem=ss(), recv_sem=rs(),
                                                device_id=to, device_id_type=MESH)

        def wait_recv(self):
            self.make().wait_recv()

        def wait_send(self):
            self.make().wait_send()

    sent = []

    ag = {}

    def ag_send(key, i, src_rows, dst_rows, cols, to):
        cp = send(lambda: U.at[src_rows, cols], lambda: U.at[dst_rows, cols], lambda: ag_s.at[i], lambda: ag_r.at[i], to)
        ag[key] = cp
        sent.append(cp)

    gw = {}

    def gw_send(key, i, src_rows, dst_rows, to):
        cp = send(lambda: GW.at[src_rows, :], lambda: GW.at[dst_rows, :], lambda: gw_s.at[i], lambda: gw_r.at[i], to)
        gw[key] = cp
        sent.append(cp)

    def a2(k):
        ag_send(("2x", k), 3 + k * 6, rows(k, 0, 0), rows(k, 0, 1), H0, xn)
        ag_send(("2y", k), 4 + k * 6, rows(k, 0, 0), rows(k, 0, 2), H1, yn)
        gw_send(("2", k), 3 + k * 3, rows(k, 0, 0), rows(k, 0, 1), xn)

    def a3(k):
        ag[("2x", k)].wait_recv()
        ag_send(("3y", k), 5 + k * 6, rows(k, 0, 0, 2), rows(k, 0, 2, 2), H0, yn)
        ag[("2y", k)].wait_recv()
        ag_send(("3x", k), 6 + k * 6, rows(k, 0, 0), rows(k, 0, 1), H1, xn)
        ag_send(("3d", k), 7 + k * 6, rows(k, 0, 2), rows(k, 0, 3), H1, xn)
        gw[("2", k)].wait_recv()
        gw_send(("3", k), 4 + k * 3, rows(k, 0, 0, 2), rows(k, 0, 2, 2), yn)

    def a4(k):
        for n in ("3y", "3x", "3d"):
            ag[(n, k)].wait_recv()
        ag_send(("4", k), 8 + k * 6, rows(k, 0, 0, 4), rows(k, 1, 0, 4), ALL, core)
        gw[("3", k)].wait_recv()
        gw_send(("4", k), 5 + k * 3, rows(k, 0, 0, 4), rows(k, 1, 0, 4), core)

    def a5(k):
        ag[("4", k)].wait_recv()
        gw[("4", k)].wait_recv()

    def zwait(k):
        ag[("z", k)].wait_recv()
        gw[("z", k)].wait_recv()
        a2(k)

    SC = jax.named_scope
    with SC("ag_start"):
        for k in (1, 2, 3):
            ag_send(("z", k), k - 1, rows(0, 0, 0), rows(k, 0, 0), ALL, zp[k])
            gw_send(("z", k), k - 1, rows(0, 0, 0), rows(k, 0, 0), zp[k])
        a2(0)
    with SC("ag_z1"):
        zwait(1)
    with SC("ag_30"):
        a3(0)
    with SC("ag_z2"):
        zwait(2)
    with SC("ag_31"):
        a3(1)
    with SC("ag_z3"):
        zwait(3)
    with SC("ag_41"):
        a4(1)
    with SC("ag_32"):
        a3(2)

    rs = {}

    def rs_send(key, i, src, dst, to):
        cp = send(src, dst, lambda: rs_s.at[i], lambda: rs_r.at[i], to)
        rs[key] = cp
        sent.append(cp)

    COLS = (H0, H1)

    def s1(k, hh):
        cs = COLS[hh]
        rs_send(("1", k, hh), k * 10 + hh, lambda: Pb.at[rows(k, 1, 0, 4), cs], lambda: R1.at[pl.ds(k * 64, 64), cs], core)

    def s2(k, hh):
        cs = COLS[hh]
        rs[("1", k, hh)].wait_recv()
        Pb[rows(k, 0, 0, 4), cs] = Pb[rows(k, 0, 0, 4), cs] + R1[pl.ds(k * 64, 64), cs]
        if hh == 0:
            rs_send(("2y", k), k * 10 + 2, lambda: Pb.at[rows(k, 0, 2, 2), H0], lambda: R2y.at[pl.ds(k * 32, 32), :], yn)
        else:
            rs_send(("2d", k), k * 10 + 3, lambda: Pb.at[rows(k, 0, 3), H1], lambda: R2x.at[pl.ds(k * 32 + 16, 16), :], xn)
            rs_send(("2x", k), k * 10 + 4, lambda: Pb.at[rows(k, 0, 1), H1], lambda: R2x.at[pl.ds(k * 32, 16), :], xn)

    def s3(k, hh):
        if hh == 0:
            rs[("2y", k)].wait_recv()
            Pb[rows(k, 0, 1), H0] = Pb[rows(k, 0, 1), H0] + R2y[pl.ds(k * 32 + 16, 16), :]
            rs_send(("3x", k), k * 10 + 5, lambda: Pb.at[rows(k, 0, 1), H0], lambda: R3x.at[pl.ds(k * 16, 16), :], xn)
            Pb[rows(k, 0, 0), H0] = Pb[rows(k, 0, 0), H0] + R2y[pl.ds(k * 32, 16), :]
        else:
            rs[("2d", k)].wait_recv()
            Pb[rows(k, 0, 2), H1] = Pb[rows(k, 0, 2), H1] + R2x[pl.ds(k * 32 + 16, 16), :]
            rs_send(("3y", k), k * 10 + 6, lambda: Pb.at[rows(k, 0, 2), H1], lambda: R3y.at[pl.ds(k * 16, 16), :], yn)
            rs[("2x", k)].wait_recv()
            Pb[rows(k, 0, 0), H1] = Pb[rows(k, 0, 0), H1] + R2x[pl.ds(k * 32, 16), :]

    def s4(k, hh):
        cs = COLS[hh]
        part = R3x if hh == 0 else R3y
        rs[("3x" if hh == 0 else "3y", k)].wait_recv()
        Pb[rows(k, 0, 0), cs] = Pb[rows(k, 0, 0), cs] + part[pl.ds(k * 16, 16), :]
        if k:
            rs_send(("4", k, hh), k * 10 + 7 + hh, lambda: Pb.at[rows(k, 0, 0), cs], lambda: R4.at[pl.ds(k * 16, 16), cs], zp[k])

    def chunk(ci, k0, n, first, hooks):
        m = n * 8 * bdev
        cr = pl.ds(k0 * 8 * bdev, m)
        mr = pl.ds(0, m)
        lanes = lax.broadcasted_iota(jnp.int32, (m, 128), 1)
        steps = (2 * nt + 2) // UNROLL

        def hook(i):
            if hooks.get(i):
                with SC(f"c{ci}_hook{i}"):
                    for fn, *a in hooks[i]:
                        fn(*a)

        def up(t):
            zz = jnp.dot(U[cr, :], W13[t], preferred_element_type=F32)
            z1, z3 = zz[:, :128], zz[:, 128:]
            g = z1 * jax.nn.sigmoid(z1) * z3
            g = jnp.where((t < 2 * nt) | (dev < SHARED_DEVS), g, 0.0)
            G[mr, pl.ds(pl.multiple_of(t * 128, 128), 128)] = g.astype(BF16)

        def ups(t, _):
            if first:
                for v in range(UNROLL):
                    got(W13.at[t * UNROLL + v], wsem.at[t * UNROLL + v])
            for v in range(UNROLL):
                up(t * UNROLL + v)
            for p in range(steps - 1):
                if hooks.get(p):
                    @pl.when(t == p)
                    def _(p=p):
                        hook(p)
            return 0

        def down(t):
            acc = jnp.dot(G[mr, pl.ds(2 * f, 256)], S2[t], preferred_element_type=F32)
            for e in range(2):
                r = jnp.dot(G[mr, pl.ds(e * f, f)], W2[t, e], preferred_element_type=F32).astype(BF16).astype(F32)
                g = GB[e, mr, :]
                g = jnp.concatenate([g, g], axis=1)
                acc = acc + jnp.where(g > 0, g * r, 0.0)
            Pb[cr, pl.ds(pl.multiple_of(t * 256, 256), 256)] = acc

        def downs(t, _):
            if first:
                for v in range(UNROLL2):
                    got(W2.at[t * UNROLL2 + v], w2sem.at[t * UNROLL2 + v])
                    got(S2.at[t * UNROLL2 + v], s2sem.at[t * UNROLL2 + v])
            for v in range(UNROLL2):
                down(t * UNROLL2 + v)

            if hooks.get(3):
                @pl.when(t == 0)
                def _():
                    hook(3)
            return 0

        with SC(f"c{ci}_gates"):
            for e in range(2):
                gv = jnp.sum(jnp.where(lanes == dev * 2 + e, GW[cr, :], 0.0), axis=1, keepdims=True)
                GB[e, mr, :] = jnp.broadcast_to(gv, (m, 128))
        with SC(f"c{ci}_up"):
            lax.fori_loop(0, steps, ups, 0)
        hook(2)
        with SC(f"c{ci}_down"):
            lax.fori_loop(0, (d // 256) // UNROLL2, downs, 0)
        hook(4)

    for ci, (k0, n) in enumerate(CHUNKS):
        for k in range(k0, k0 + n):
            with SC(f"c{ci}_a5"):
                a5(k)
        chunk(ci, k0, n, ci == 0, HOOKS(ci, a2, zwait, a3, a4, a5, s1, s2, s3, s4))
    ka, kb = CHUNKS[-2][0], CHUNKS[-1][0]
    with SC("t_s2"):
        s2(kb, 0)
        s2(kb, 1)
    with SC("t_s4a"):
        s4(ka, 0)
        s4(ka, 1)
    with SC("t_s3"):
        s3(kb, 0)
        s3(kb, 1)
    with SC("t_s4"):
        s4(kb, 0)
        s4(kb, 1)

    acc = h_ref[...].astype(F32) + Pb[rows(0, 0, 0), :]
    for k in (1, 2, 3):
        with SC(f"t_s5{k}"):
            rs[("4", k, 0)].wait_recv()
            rs[("4", k, 1)].wait_recv()
        acc = acc + R4[pl.ds(k * 16, 16), :]
    y_ref[...] = acc.astype(BF16)
    for cp in sent:
        cp.wait_send()


def solution(mesh):
    def body(x, kv_k, kv_v, lens, idx, gates, ln1, wq, wo, ln2, ws1, ws3, ws2, w1, w3, w2):
        bdev, d = x.shape
        f = w1.shape[2]
        rows = bdev * 32
        h = _attention_block(x, kv_k, kv_v, lens, ln1, wq, wo)
        vm = pl.BlockSpec(memory_space=pltpu.VMEM)
        hbm = pl.BlockSpec(memory_space=pl.ANY)
        mmax = max(n for _, n in CHUNKS) * 8 * bdev
        return pl.pallas_call(
            _moe_kernel,
            out_shape=jax.ShapeDtypeStruct((bdev, d), BF16),
            in_specs=[vm] * 4 + [hbm] * 6,
            out_specs=vm,
            scratch_shapes=[
                pltpu.VMEM((rows, d), BF16),
                pltpu.VMEM((rows, 128), F32),
                pltpu.VMEM((2, mmax, 128), F32),
                pltpu.VMEM((rows, d), F32),
                pltpu.VMEM((rows // 2, d), F32),
                pltpu.VMEM((128, d // 2), F32),
                pltpu.VMEM((128, d // 2), F32),
                pltpu.VMEM((64, d // 2), F32),
                pltpu.VMEM((64, d // 2), F32),
                pltpu.VMEM((64, d), F32),
                pltpu.VMEM((mmax, 2 * f + 256), BF16),
                pltpu.VMEM((2 * f // 128 + 2, d, 256), BF16),
                pltpu.VMEM((d // 256, 2, f, 256), BF16),
                pltpu.VMEM((d // 256, 256, 256), BF16),
                pltpu.SemaphoreType.DMA((2 * f // 128 + 2,)),
                pltpu.SemaphoreType.DMA((d // 256,)),
                pltpu.SemaphoreType.DMA((d // 256,)),
                pltpu.SemaphoreType.DMA((28,)),
                pltpu.SemaphoreType.DMA((28,)),
                pltpu.SemaphoreType.DMA((16,)),
                pltpu.SemaphoreType.DMA((16,)),
                pltpu.SemaphoreType.DMA((40,)),
                pltpu.SemaphoreType.DMA((40,)),
            ],
            compiler_params=pltpu.CompilerParams(
                collective_id=0, has_side_effects=True, vmem_limit_bytes=60 * 1024 * 1024
            ),
        )(h, ln2.reshape(1, d), idx, gates, ws1, ws3, ws2, w1, w3, w2)

    rows = P(GRP)
    rep = P()
    return jax.shard_map(
        body, mesh=mesh,
        in_specs=(rows, rows, rows, rows, rows, rows, rep, rep, rep, rep, rep, rep, rep, rows, rows, rows),
        out_specs=rows, check_vma=False)
```

```python
import functools

import jax
import jax.numpy as jnp
from jax import lax
from jax.experimental import pallas as pl
from jax.experimental.pallas import tpu as pltpu
from jax.sharding import PartitionSpec as P

EPS = 1e-6
GRP = ("ey", "ex")
MESH = pl.DeviceIdType.MESH
BF16, F32 = jnp.bfloat16, jnp.float32

LANES, TILE = 128, 256


def _loop(n, step):
    def body(t, carry):
        step(t)
        return carry
    lax.fori_loop(0, n, body, 0)


def _at(t, width):
    return pl.ds(pl.multiple_of(t * width, width), width)


SHARED_DEVS = 22
CHUNKS = ((1, 1), (2, 1), (3, 1), (0, 1))
UNROLL, UNROLL2 = 8, 4


def HOOKS(ci, a2, zwait, a3, a4, a5, s1, s2, s3, s4):
    order = [k for k, _ in CHUNKS]
    k = order[ci]
    ev = {i: [] for i in range(5)}
    if ci == 0:
        ev[1] += [(a3, 3), (a4, 2)]
        ev[2] += [(a4, 0)]
        ev[4] += [(a4, 3)]
    if ci >= 2:
        ev[1] += [(s4, order[ci - 2], 0), (s4, order[ci - 2], 1)]
    if ci >= 1:
        ev[0] += [(s2, order[ci - 1], 0), (s2, order[ci - 1], 1)]
    ev[3] += [(s1, k, 0)]
    ev[4] += [(s1, k, 1)]
    if ci >= 1:
        ev[4] += [(s3, order[ci - 1], 0), (s3, order[ci - 1], 1)]
    return ev


def _norm(v, ln_ref):
    r = lax.rsqrt(jnp.mean(v * v, axis=-1, keepdims=True) + EPS)
    n = v.shape[1] // 128
    return jnp.concatenate(
        [(v[:, i * 128:(i + 1) * 128] * r * ln_ref[i:i + 1, :].astype(F32)).astype(BF16) for i in range(n)], axis=1)


def _attend(lens_ref, x_ref, ln1_ref, ln2_ref, k_hbm, v_hbm, wq_hbm, wo_hbm, h_ref, u_ref, between,
            WQ, WO, K, V, QS, OS, A, ACC, POS, qsem, osem, ksem, vsem):
    b, d = x_ref.shape
    hd = LANES
    nh = wq_hbm.shape[1] // hd
    rows = K.shape[1]
    kvh = rows // 256
    grp = nh // kvh
    nq, no, nk = qsem.shape[0], osem.shape[0], ksem.shape[0]
    cq, co, ck = d // nq, (nh * hd) // no, b // nk

    def cpq(i):
        return pltpu.make_async_copy(wq_hbm.at[_at(i, cq), :], WQ.at[_at(i, cq), :], qsem.at[i])

    def cpo(i):
        return pltpu.make_async_copy(wo_hbm.at[_at(i, co), :], WO.at[_at(i, co), :], osem.at[i])

    def cpk(i):
        return pltpu.make_async_copy(k_hbm.at[pl.ds(i * ck, ck)], K.at[pl.ds(i * ck, ck)], ksem.at[i])

    def cpv(i):
        return pltpu.make_async_copy(v_hbm.at[pl.ds(i * ck, ck)], V.at[pl.ds(i * ck, ck)], vsem.at[i])

    _loop(nq, lambda i: cpq(i).start())
    xf = x_ref[...].astype(F32)
    A[...] = _norm(xf, ln1_ref)
    ACC[...] = jnp.zeros(ACC.shape, F32)
    row = lax.broadcasted_iota(jnp.int32, (rows, LANES), 0)
    lane = lax.broadcasted_iota(jnp.int32, (rows, LANES), 1)
    own = lax.rem(row, kvh) == lax.div(lax.rem(lane, nh), grp)
    POS[...] = jnp.where(own, lax.div(row, kvh), 1 << 20)
    between[0]()

    def queries(i):
        cpq(i).wait()

        @pl.when(i >= nq - nk)
        def _():
            cpk(i - (nq - nk)).start()
            cpv(i - (nq - nk)).start()
        ACC[...] = ACC[...] + jnp.dot(A[:, _at(i, cq)], WQ[_at(i, cq), :], preferred_element_type=F32)
    _loop(nq, queries)
    _loop(no, lambda i: cpo(i).start())
    for i in range(nh):
        QS[i * b:(i + 1) * b, :] = ACC[:, i * hd:(i + 1) * hd].astype(BF16).astype(F32)
    between[1]()

    lane1 = lax.div(lax.broadcasted_iota(jnp.int32, (1, LANES), 1), nh)
    slot = lax.div(lax.broadcasted_iota(jnp.int32, (LANES, LANES), 1), nh)
    scale = hd ** -0.5 * 1.4426950408889634

    def group(g):
        cpk(g).wait()
        cpv(g).wait()
        first = g * ck
        q = jnp.concatenate([QS[pl.ds(first + i, nh, stride=b), :] for i in range(ck)], axis=0)
        qt = jnp.transpose(q)
        qq = jnp.concatenate([jnp.where(slot == i, qt, 0.0).astype(BF16) for i in range(ck)], axis=0)
        kc = jnp.concatenate([K[first + i] for i in range(ck)], axis=1)
        s = jnp.dot(kc, qq, preferred_element_type=F32)
        n = jnp.zeros(lane1.shape, jnp.int32)
        for i in range(ck):
            n = jnp.where(lane1 == i, lens_ref[first + i], n)
        s = jnp.where(POS[...] < n, s, -jnp.inf)
        p = jnp.exp2((s - jnp.max(s, axis=0, keepdims=True)) * scale)
        p = (p * (1.0 / jnp.sum(p, axis=0, keepdims=True))).astype(BF16)
        pt = jnp.transpose(p)
        for i in range(ck):
            o = jnp.dot(pt[i * nh:(i + 1) * nh, :], V[first + i], preferred_element_type=F32)
            OS[pl.ds(first + i, nh, stride=b), :] = o.astype(BF16).astype(F32)
    _loop(nk, group)
    between[2]()

    ACC[:, 0:d] = jnp.zeros((b, d), F32)

    def outs(i):
        cpo(i).wait()
        n = co // hd
        o = jnp.concatenate([OS[pl.ds(pl.multiple_of((i * n + j) * b, b), b), :].astype(BF16) for j in range(n)], axis=1)
        ACC[:, 0:d] = ACC[:, 0:d] + jnp.dot(o, WO[_at(i, co), :], preferred_element_type=F32)
    _loop(no, outs)
    h = (xf + ACC[:, 0:d]).astype(BF16)
    h_ref[...] = h
    u_ref[...] = _norm(h.astype(F32), ln2_ref)


def _gates(idx_ref, gate_ref, gw_ref, IDX, GT):
    top, b = idx_ref.shape
    cap = b - b // 8
    IDX[...] = jnp.zeros(IDX.shape, jnp.int32)
    GT[...] = jnp.zeros(GT.shape, F32)
    IDX[0:top, 0:b] = idx_ref[...]
    GT[0:top, 0:b] = gate_ref[...]
    expert = lax.broadcasted_iota(jnp.int32, (LANES, LANES), 0)
    oh = jnp.zeros((LANES, LANES), F32)
    gm = jnp.zeros((LANES, LANES), F32)
    for j in range(top):
        hit = IDX[j:j + 1, :] == expert
        oh = oh + jnp.where(hit, 1.0, 0.0)
        gm = gm + jnp.where(hit, GT[j:j + 1, :], 0.0)
    before = jnp.where(expert < lax.broadcasted_iota(jnp.int32, (LANES, LANES), 1), 1.0, 0.0)
    rank = jnp.dot(oh.astype(BF16), before.astype(BF16), preferred_element_type=F32)
    gw_ref[...] = jnp.transpose(jnp.where(rank < cap - 0.5, gm, 0.0))[0:b, :]


def _layer_kernel(lens_ref, x_ref, ln1_ref, ln2_ref, idx_ref, gate_ref, k_hbm, v_hbm, wq_hbm, wo_hbm,
                  s1_hbm, s3_hbm, s2_hbm, w1_hbm, w3_hbm, w2_hbm, y_ref, h_ref, IDX, GT,
                  U, GW, R1, R2x, R2y, R3x, R3y, R4,
                  ag_s, ag_r, gw_s, gw_r, rs_s, rs_r):
    z = lax.axis_index("ey")
    ex = lax.axis_index("ex")
    c = lax.rem(ex, 2)
    xx = lax.rem(lax.div(ex, 2), 2)
    yy = lax.div(ex, 4)
    dev = z * 8 + ex
    bdev, d = x_ref.shape
    f = w1_hbm.shape[2]
    half = d // 2
    H0, H1 = pl.ds(0, half), pl.ds(half, half)
    ALL = pl.ds(0, d)
    core = (z, ex + 1 - 2 * c)
    xn = (z, ex + 2 - 4 * xx)
    yn = (z, ex + 4 - 8 * yy)
    zp = {1: (z + 1 - 2 * lax.rem(z, 2), ex), 2: (z + 2 - 4 * lax.div(z, 2), ex), 3: (3 - z, ex)}

    def rows(k, dc, dq, n=1):
        return pl.ds(((k * 2 + dc) * 4 + dq) * bdev, n * bdev)

    _gates(idx_ref, gate_ref, GW.at[rows(0, 0, 0), :], IDX, GT)

    SC0 = jax.named_scope
    barrier = pltpu.get_barrier_semaphore()
    for n in (core, xn, yn, zp[1], zp[2], zp[3]):
        pl.semaphore_signal(barrier, inc=1, device_id=n, device_id_type=MESH)
    with SC0("barrier"):
        pl.semaphore_wait(barrier, 6)

    class send:
        def __init__(self, *args):
            self.args = args
            self.make().start()

        def make(self):
            src, dst, ss, rs, to = self.args
            return pltpu.make_async_remote_copy(src_ref=src(), dst_ref=dst(), send_sem=ss(), recv_sem=rs(),
                                                device_id=to, device_id_type=MESH)

        def wait_recv(self):
            self.make().wait_recv()

        def wait_send(self):
            self.make().wait_send()

    sent = []

    def flush():
        for cp in sent:
            cp.wait_send()
        sent.clear()

    ag = {}

    def ag_send(key, i, src_rows, dst_rows, cols, to):
        cp = send(lambda: U.at[src_rows, cols], lambda: U.at[dst_rows, cols], lambda: ag_s.at[i], lambda: ag_r.at[i], to)
        ag[key] = cp
        sent.append(cp)

    gw = {}

    def gw_send(key, i, src_rows, dst_rows, to):
        cp = send(lambda: GW.at[src_rows, :], lambda: GW.at[dst_rows, :], lambda: gw_s.at[i], lambda: gw_r.at[i], to)
        gw[key] = cp
        sent.append(cp)

    def a2(k, hh):
        cs = (H0, H1)[hh]
        near, far = (xn, yn) if hh == 0 else (yn, xn)
        nd, fd = (1, 2) if hh == 0 else (2, 1)
        ag_send(("2", k, hh), 6 + k * 8 + hh, rows(k, 0, 0), rows(k, 0, nd), cs, near)
        ag_send(("3", k, hh), 8 + k * 8 + hh, rows(k, 0, 0), rows(k, 0, fd), cs, far)

    def g1():
        for k in (1, 2, 3):
            gw_send(("z", k), k - 1, rows(0, 0, 0), rows(k, 0, 0), zp[k])

    def g2():
        for k in range(4):
            if k:
                gw[("z", k)].wait_recv()
            gw_send(("2", k), 3 + k * 3, rows(k, 0, 0), rows(k, 0, 1), xn)

    def g3():
        for k in range(4):
            gw[("2", k)].wait_recv()
            gw_send(("3", k), 4 + k * 3, rows(k, 0, 0, 2), rows(k, 0, 2, 2), yn)

    def g4():
        for k in range(4):
            gw[("3", k)].wait_recv()
            gw_send(("4", k), 5 + k * 3, rows(k, 0, 0, 4), rows(k, 1, 0, 4), core)

    def a3(k):
        ag[("2", k, 0)].wait_recv()
        ag_send(("4", k, 0), 10 + k * 8, rows(k, 0, 1), rows(k, 0, 3), H0, yn)
        ag[("2", k, 1)].wait_recv()
        ag_send(("4", k, 1), 11 + k * 8, rows(k, 0, 2), rows(k, 0, 3), H1, xn)

    def a4(k):
        for hh in range(2):
            ag[("3", k, hh)].wait_recv()
        ag_send(("5", k), 12 + k * 8, rows(k, 0, 0, 3), rows(k, 1, 0, 3), ALL, core)
        for hh in range(2):
            ag[("4", k, hh)].wait_recv()
        ag_send(("6", k), 13 + k * 8, rows(k, 0, 3), rows(k, 1, 3), ALL, core)

    def a5(k):
        ag[("5", k)].wait_recv()
        ag[("6", k)].wait_recv()

    def zwait(k):
        for hh in range(2):
            ag[("z", k, hh)].wait_recv()
            a2(k, hh)

    nh, l4 = wq_hbm.shape[1] // LANES, k_hbm.shape[1]
    pl.run_scoped(
        functools.partial(_attend, lens_ref, x_ref, ln1_ref, ln2_ref, k_hbm, v_hbm, wq_hbm, wo_hbm, h_ref,
                          U.at[rows(0, 0, 0), :], (g1, g2, g3)),
        pltpu.VMEM(wq_hbm.shape, BF16),
        pltpu.VMEM(wo_hbm.shape, BF16),
        pltpu.VMEM(k_hbm.shape, BF16),
        pltpu.VMEM(k_hbm.shape, BF16),
        pltpu.VMEM((nh * bdev, LANES), F32),
        pltpu.VMEM((nh * bdev, LANES), F32),
        pltpu.VMEM((bdev, d), BF16),
        pltpu.VMEM((bdev, nh * LANES), F32),
        pltpu.VMEM((l4, LANES), jnp.int32),
        pltpu.SemaphoreType.DMA((8,)),
        pltpu.SemaphoreType.DMA((8,)),
        pltpu.SemaphoreType.DMA((4,)),
        pltpu.SemaphoreType.DMA((4,)),
    )

    def experts(GB, Pb, G, W13, W2, S2, wsem, w2sem, s2sem):
        with SC0("ag_start"):
            for k in (1, 2, 3):
                for hh in range(2):
                    ag_send(("z", k, hh), (k - 1) * 2 + hh, rows(0, 0, 0), rows(k, 0, 0), (H0, H1)[hh], zp[k])
            a2(0, 0)
            a2(0, 1)
        nt = f // 128
        L0, L1 = pl.ds(0, LANES), pl.ds(LANES, LANES)

        def load(src, dst, sem):
            pltpu.make_async_copy(src, dst, sem).start()

        def load13(a, b, e, base, count):
            def step(t):
                col = _at(t, LANES)
                load(a.at[e, :, col], W13.at[base + t, :, L0], wsem.at[base + t])
                load(b.at[e, :, col], W13.at[base + t, :, L1], wsem.at[base + t])
            _loop(count, step)

        load13(w1_hbm, w3_hbm, 0, 0, nt)
        load13(w1_hbm, w3_hbm, 1, nt, nt)
        sbase = lax.rem(dev, SHARED_DEVS) * 2
        for t in range(2):
            col = _at(sbase + t, LANES)
            load(s1_hbm.at[:, col], W13.at[2 * nt + t, :, L0], wsem.at[2 * nt + t])
            load(s3_hbm.at[:, col], W13.at[2 * nt + t, :, L1], wsem.at[2 * nt + t])
        scol = _at(sbase // 2, TILE)

        def load2(t):
            col = _at(t, TILE)
            for e in range(2):
                load(w2_hbm.at[e, :, col], W2.at[t, e], w2sem.at[t])
            load(s2_hbm.at[scol, col], S2.at[t], s2sem.at[t])
        _loop(d // TILE, load2)

        def got(ref, sem):
            pltpu.make_async_copy(ref, ref, sem).wait()

        g4()
        with SC0("ag_z1"):
            zwait(1)
        with SC0("ag_30"):
            a3(0)
        with SC0("ag_z2"):
            zwait(2)
        with SC0("ag_31"):
            a3(1)
        with SC0("ag_z3"):
            zwait(3)
        with SC0("ag_41"):
            a4(1)
        with SC0("ag_32"):
            a3(2)

        rs = {}

        def rs_send(key, i, src, dst, to):
            cp = send(src, dst, lambda: rs_s.at[i], lambda: rs_r.at[i], to)
            rs[key] = cp
            sent.append(cp)

        COLS = (H0, H1)

        def s1(k, hh):
            cs = COLS[hh]
            rs_send(("1", k, hh), k * 10 + hh, lambda: Pb.at[rows(k, 1, 0, 4), cs], lambda: R1.at[pl.ds(k * 64, 64), cs], core)

        def s2(k, hh):
            cs = COLS[hh]
            rs[("1", k, hh)].wait_recv()
            Pb[rows(k, 0, 0, 4), cs] = Pb[rows(k, 0, 0, 4), cs] + R1[pl.ds(k * 64, 64), cs]
            if hh == 0:
                rs_send(("2y", k), k * 10 + 2, lambda: Pb.at[rows(k, 0, 2, 2), H0], lambda: R2y.at[pl.ds(k * 32, 32), :], yn)
            else:
                rs_send(("2d", k), k * 10 + 3, lambda: Pb.at[rows(k, 0, 3), H1], lambda: R2x.at[pl.ds(k * 32 + 16, 16), :], xn)
                rs_send(("2x", k), k * 10 + 4, lambda: Pb.at[rows(k, 0, 1), H1], lambda: R2x.at[pl.ds(k * 32, 16), :], xn)

        def s3(k, hh):
            if hh == 0:
                rs[("2y", k)].wait_recv()
                Pb[rows(k, 0, 1), H0] = Pb[rows(k, 0, 1), H0] + R2y[pl.ds(k * 32 + 16, 16), :]
                rs_send(("3x", k), k * 10 + 5, lambda: Pb.at[rows(k, 0, 1), H0], lambda: R3x.at[pl.ds(k * 16, 16), :], xn)
                Pb[rows(k, 0, 0), H0] = Pb[rows(k, 0, 0), H0] + R2y[pl.ds(k * 32, 16), :]
            else:
                rs[("2d", k)].wait_recv()
                Pb[rows(k, 0, 2), H1] = Pb[rows(k, 0, 2), H1] + R2x[pl.ds(k * 32 + 16, 16), :]
                rs_send(("3y", k), k * 10 + 6, lambda: Pb.at[rows(k, 0, 2), H1], lambda: R3y.at[pl.ds(k * 16, 16), :], yn)
                rs[("2x", k)].wait_recv()
                Pb[rows(k, 0, 0), H1] = Pb[rows(k, 0, 0), H1] + R2x[pl.ds(k * 32, 16), :]

        def s4(k, hh):
            cs = COLS[hh]
            part = R3x if hh == 0 else R3y
            rs[("3x" if hh == 0 else "3y", k)].wait_recv()
            Pb[rows(k, 0, 0), cs] = Pb[rows(k, 0, 0), cs] + part[pl.ds(k * 16, 16), :]
            if k:
                rs_send(("4", k, hh), k * 10 + 7 + hh, lambda: Pb.at[rows(k, 0, 0), cs], lambda: R4.at[pl.ds(k * 16, 16), cs], zp[k])

        SC = jax.named_scope
        def chunk(ci, k0, n, first, hooks):
            m = n * 8 * bdev
            cr = pl.ds(k0 * 8 * bdev, m)
            mr = pl.ds(0, m)
            lanes = lax.broadcasted_iota(jnp.int32, (m, LANES), 1)
            steps = (2 * nt + 2) // UNROLL

            def hook(i):
                if hooks.get(i):
                    with SC(f"c{ci}_hook{i}"):
                        for fn, *a in hooks[i]:
                            fn(*a)

            def up(t):
                zz = jnp.dot(U[cr, :], W13[t], preferred_element_type=F32)
                z1, z3 = zz[:, :128], zz[:, 128:]
                g = z1 * jax.nn.sigmoid(z1) * z3
                g = jnp.where((t < 2 * nt) | (dev < SHARED_DEVS), g, 0.0)
                G[mr, _at(t, LANES)] = g.astype(BF16)

            def ups(t):
                if first:
                    for v in range(UNROLL):
                        got(W13.at[t * UNROLL + v], wsem.at[t * UNROLL + v])
                for v in range(UNROLL):
                    up(t * UNROLL + v)
                for p in range(steps - 1):
                    if hooks.get(p):
                        @pl.when(t == p)
                        def _(p=p):
                            hook(p)

            def down(t):
                acc = jnp.dot(G[mr, pl.ds(2 * f, 256)], S2[t], preferred_element_type=F32)
                for e in range(2):
                    r = jnp.dot(G[mr, pl.ds(e * f, f)], W2[t, e], preferred_element_type=F32).astype(BF16).astype(F32)
                    g = GB[e, mr, :]
                    g = jnp.concatenate([g, g], axis=1)
                    acc = acc + jnp.where(g > 0, g * r, 0.0)
                Pb[cr, _at(t, TILE)] = acc

            def downs(t):
                if first:
                    for v in range(UNROLL2):
                        got(W2.at[t * UNROLL2 + v], w2sem.at[t * UNROLL2 + v])
                        got(S2.at[t * UNROLL2 + v], s2sem.at[t * UNROLL2 + v])
                for v in range(UNROLL2):
                    down(t * UNROLL2 + v)

                if hooks.get(3):
                    @pl.when(t == 0)
                    def _():
                        hook(3)

            with SC(f"c{ci}_gates"):
                for e in range(2):
                    gv = jnp.sum(jnp.where(lanes == dev * 2 + e, GW[cr, :], 0.0), axis=1, keepdims=True)
                    GB[e, mr, :] = jnp.broadcast_to(gv, (m, LANES))
            with SC(f"c{ci}_up"):
                _loop(steps, ups)
            if ci == len(CHUNKS) - 1:
                flush()
            hook(2)
            with SC(f"c{ci}_down"):
                _loop(d // TILE // UNROLL2, downs)
            hook(4)

        for ci, (k0, n) in enumerate(CHUNKS):
            for k in range(k0, k0 + n):
                with SC(f"c{ci}_a5"):
                    a5(k)
                    gw[("4", k)].wait_recv()
            chunk(ci, k0, n, ci == 0, HOOKS(ci, a2, zwait, a3, a4, a5, s1, s2, s3, s4))
        ka, kb = CHUNKS[-2][0], CHUNKS[-1][0]
        with SC("t_s2"):
            s2(kb, 0)
            s2(kb, 1)
        with SC("t_s4a"):
            s4(ka, 0)
            s4(ka, 1)
        with SC("t_s3"):
            s3(kb, 0)
            s3(kb, 1)
        with SC("t_s4"):
            s4(kb, 0)
            s4(kb, 1)

        acc = h_ref[...].astype(F32) + Pb[rows(0, 0, 0), :]
        for k in (1, 2, 3):
            with SC(f"t_s5{k}"):
                rs[("4", k, 0)].wait_recv()
                rs[("4", k, 1)].wait_recv()
            acc = acc + R4[pl.ds(k * 16, 16), :]
        y_ref[...] = acc.astype(BF16)
        flush()

    mmax = max(n for _, n in CHUNKS) * 8 * bdev
    f = w1_hbm.shape[2]
    pl.run_scoped(
        experts,
        pltpu.VMEM((2, mmax, LANES), F32),
        pltpu.VMEM((bdev * 32, d), F32),
        pltpu.VMEM((mmax, 2 * f + TILE), BF16),
        pltpu.VMEM((2 * f // LANES + 2, d, TILE), BF16),
        pltpu.VMEM((d // TILE, 2, f, TILE), BF16),
        pltpu.VMEM((d // TILE, TILE, TILE), BF16),
        pltpu.SemaphoreType.DMA((2 * f // LANES + 2,)),
        pltpu.SemaphoreType.DMA((d // TILE,)),
        pltpu.SemaphoreType.DMA((d // TILE,)),
    )


def solution(mesh):
    def body(x, kv_k, kv_v, lens, idx, gates, ln1, wq, wo, ln2, ws1, ws3, ws2, w1, w3, w2):
        bdev, d = x.shape
        _, l, kvh, hd = kv_k.shape
        rows = bdev * 32
        vm = pl.BlockSpec(memory_space=pltpu.VMEM)
        hbm = pl.BlockSpec(memory_space=pl.ANY)
        kv = (bdev, l * kvh, hd)
        sem = pltpu.SemaphoreType.DMA
        return pl.pallas_call(
            _layer_kernel,
            out_shape=jax.ShapeDtypeStruct((bdev, d), BF16),
            in_specs=[pl.BlockSpec(memory_space=pltpu.SMEM)] + [vm] * 5 + [hbm] * 10,
            out_specs=vm,
            scratch_shapes=[
                pltpu.VMEM((bdev, d), BF16),
                pltpu.VMEM((8, LANES), jnp.int32),
                pltpu.VMEM((8, LANES), F32),
                pltpu.VMEM((rows, d), BF16),
                pltpu.VMEM((rows, LANES), F32),
                pltpu.VMEM((rows // 2, d), F32),
                pltpu.VMEM((rows // 4, d // 2), F32),
                pltpu.VMEM((rows // 4, d // 2), F32),
                pltpu.VMEM((rows // 8, d // 2), F32),
                pltpu.VMEM((rows // 8, d // 2), F32),
                pltpu.VMEM((rows // 8, d), F32),
                sem((38,)), sem((38,)), sem((16,)), sem((16,)), sem((40,)), sem((40,)),
            ],
            compiler_params=pltpu.CompilerParams(
                collective_id=0, has_side_effects=True, vmem_limit_bytes=62 * 1024 * 1024
            ),
        )(lens, x, ln1.reshape(d // LANES, LANES), ln2.reshape(d // LANES, LANES), idx.T, gates.T,
          kv_k.reshape(kv), kv_v.reshape(kv), wq, wo, ws1, ws3, ws2, w1, w3, w2)

    rows = P(GRP)
    rep = P()
    return jax.shard_map(
        body, mesh=mesh,
        in_specs=(rows, rows, rows, rows, rows, rows, rep, rep, rep, rep, rep, rep, rep, rows, rows, rows),
        out_specs=rows, check_vma=False)
```

```python
import functools

import jax
import jax.numpy as jnp
from jax import lax
from jax.experimental import pallas as pl
from jax.experimental.pallas import tpu as pltpu
from jax.sharding import PartitionSpec as P

EPS = 1e-6
GRP = ("ey", "ex")
MESH = pl.DeviceIdType.MESH
BF16, F32 = jnp.bfloat16, jnp.float32

LANES, TILE = 128, 256


def _loop(n, step):
    def body(t, carry):
        step(t)
        return carry
    lax.fori_loop(0, n, body, 0)


def _at(t, width):
    return pl.ds(pl.multiple_of(t * width, width), width)


SHARED_DEVS = 22
CHUNKS = ((1, 1), (2, 1), (3, 1), (0, 1))
UNROLL, UNROLL2, PAIR = 12, 8, 1


def HOOKS(ci, a2, zwait, a3, a4, a5, s1, s2, s3, s4):
    order = [k for k, _ in CHUNKS]
    k = order[ci]
    ev = {i: [] for i in range(5)}
    if ci == 0:
        ev[0] += [(a3, 3), (a4, 2)]
        ev[2] += [(a4, 0)]
        ev[4] += [(a4, 3)]
    if ci >= 2:
        ev[2] += [(s4, order[ci - 2], 0), (s4, order[ci - 2], 1)]
    if ci >= 1:
        ev[0] += [(s2, order[ci - 1], 0), (s2, order[ci - 1], 1)]
    ev[3] += [(s1, k, 0)]
    ev[4] += [(s1, k, 1)]
    if ci >= 1:
        ev[4] += [(s3, order[ci - 1], 0), (s3, order[ci - 1], 1)]
    return ev


def _norm(v, ln_ref):
    r = lax.rsqrt(jnp.mean(v * v, axis=-1, keepdims=True) + EPS)
    n = v.shape[1] // 128
    return jnp.concatenate(
        [(v[:, i * 128:(i + 1) * 128] * r * ln_ref[i:i + 1, :].astype(F32)).astype(BF16) for i in range(n)], axis=1)


def _attend(lens_ref, x_ref, ln1_ref, ln2_ref, k_hbm, v_hbm, wq_hbm, wo_hbm, h_ref, u_ref, between,
            WQ, WO, K, V, QS, OS, A, ACC, POS, qsem, osem, ksem, vsem):
    b, d = x_ref.shape
    hd = LANES
    nh = wq_hbm.shape[1] // hd
    rows = K.shape[1]
    kvh = rows // 256
    grp = nh // kvh
    nq, no, nk = qsem.shape[0], osem.shape[0], ksem.shape[0]
    cq, co, ck = d // nq, (nh * hd) // no, b // nk

    def cpq(i):
        return pltpu.make_async_copy(wq_hbm.at[_at(i, cq), :], WQ.at[_at(i, cq), :], qsem.at[i])

    def cpo(i):
        return pltpu.make_async_copy(wo_hbm.at[_at(i, co), :], WO.at[_at(i, co), :], osem.at[i])

    def cpk(i):
        return pltpu.make_async_copy(k_hbm.at[pl.ds(i * ck, ck)], K.at[pl.ds(i * ck, ck)], ksem.at[i])

    def cpv(i):
        return pltpu.make_async_copy(v_hbm.at[pl.ds(i * ck, ck)], V.at[pl.ds(i * ck, ck)], vsem.at[i])

    _loop(nq, lambda i: cpq(i).start())
    xf = x_ref[...].astype(F32)
    A[...] = _norm(xf, ln1_ref)
    ACC[...] = jnp.zeros(ACC.shape, F32)
    row = lax.broadcasted_iota(jnp.int32, (rows, LANES), 0)
    lane = lax.broadcasted_iota(jnp.int32, (rows, LANES), 1)
    own = lax.rem(row, kvh) == lax.div(lax.rem(lane, nh), grp)
    POS[...] = jnp.where(own, lax.div(row, kvh), 1 << 20)
    between[0]()

    def queries(i):
        cpq(i).wait()

        @pl.when(i >= nq - nk)
        def _():
            cpk(i - (nq - nk)).start()
            cpv(i - (nq - nk)).start()
        ACC[...] = ACC[...] + jnp.dot(A[:, _at(i, cq)], WQ[_at(i, cq), :], preferred_element_type=F32)
    _loop(nq, queries)
    _loop(no, lambda i: cpo(i).start())
    for i in range(nh):
        QS[i * b:(i + 1) * b, :] = ACC[:, i * hd:(i + 1) * hd].astype(BF16).astype(F32)
    between[1]()

    lane1 = lax.div(lax.broadcasted_iota(jnp.int32, (1, LANES), 1), nh)
    slot = lax.div(lax.broadcasted_iota(jnp.int32, (LANES, LANES), 1), nh)
    scale = hd ** -0.5 * 1.4426950408889634

    def group(g):
        first = g * ck
        q = jnp.concatenate([QS[pl.ds(first + i, nh, stride=b), :] for i in range(ck)], axis=0)
        qt = jnp.transpose(q)
        qq = jnp.concatenate([jnp.where(slot == i, qt, 0.0).astype(BF16) for i in range(ck)], axis=0)
        kc = jnp.concatenate([K[first + i] for i in range(ck)], axis=1)
        s = jnp.dot(kc, qq, preferred_element_type=F32)
        n = jnp.zeros(lane1.shape, jnp.int32)
        for i in range(ck):
            n = jnp.where(lane1 == i, lens_ref[first + i], n)
        s = jnp.where(POS[...] < n, s, -jnp.inf)
        p = jnp.exp2((s - jnp.max(s, axis=0, keepdims=True)) * scale)
        p = (p * (1.0 / jnp.sum(p, axis=0, keepdims=True))).astype(BF16)
        pt = jnp.transpose(p)
        for i in range(ck):
            o = jnp.dot(pt[i * nh:(i + 1) * nh, :], V[first + i], preferred_element_type=F32)
            OS[pl.ds(first + i, nh, stride=b), :] = o.astype(BF16).astype(F32)
    def groups(t):
        for g in range(PAIR):
            cpk(t * PAIR + g).wait()
            cpv(t * PAIR + g).wait()
        for g in range(PAIR):
            group(t * PAIR + g)
    _loop(nk // PAIR, groups)
    between[2]()

    ACC[:, 0:d] = jnp.zeros((b, d), F32)

    for i in range(no):
        cpo(i).wait()

    def outs(t):
        n = co // hd
        part = ACC[:, 0:d]
        for v in range(no // 2):
            i = t * (no // 2) + v
            o = jnp.concatenate([OS[_at(i * n + j, b), :].astype(BF16) for j in range(n)], axis=1)
            part = part + jnp.dot(o, WO[_at(i, co), :], preferred_element_type=F32)
        ACC[:, 0:d] = part
    _loop(2, outs)
    h = (xf + ACC[:, 0:d]).astype(BF16)
    h_ref[...] = h
    u_ref[...] = _norm(h.astype(F32), ln2_ref)


def _gates(idx_ref, gate_ref, gw_ref, IDX, GT):
    top, b = idx_ref.shape
    cap = b - b // 8
    IDX[...] = jnp.zeros(IDX.shape, jnp.int32)
    GT[...] = jnp.zeros(GT.shape, F32)
    IDX[0:top, 0:b] = idx_ref[...]
    GT[0:top, 0:b] = gate_ref[...]
    expert = lax.broadcasted_iota(jnp.int32, (LANES, LANES), 0)
    oh = jnp.zeros((LANES, LANES), F32)
    gm = jnp.zeros((LANES, LANES), F32)
    for j in range(top):
        hit = IDX[j:j + 1, :] == expert
        oh = oh + jnp.where(hit, 1.0, 0.0)
        gm = gm + jnp.where(hit, GT[j:j + 1, :], 0.0)
    before = jnp.where(expert < lax.broadcasted_iota(jnp.int32, (LANES, LANES), 1), 1.0, 0.0)
    rank = jnp.dot(oh.astype(BF16), before.astype(BF16), preferred_element_type=F32)
    gw_ref[...] = jnp.transpose(jnp.where(rank < cap - 0.5, gm, 0.0))[0:b, :]


def _layer_kernel(lens_ref, x_ref, ln1_ref, ln2_ref, idx_ref, gate_ref, k_hbm, v_hbm, wq_hbm, wo_hbm,
                  s1_hbm, s3_hbm, s2_hbm, w1_hbm, w3_hbm, w2_hbm, y_ref, h_ref, IDX, GT,
                  U, GW, R1, R2x, R2y, R3x, R3y, R4,
                  ag_s, ag_r, gw_s, gw_r, rs_s, rs_r):
    z = lax.axis_index("ey")
    ex = lax.axis_index("ex")
    c = lax.rem(ex, 2)
    xx = lax.rem(lax.div(ex, 2), 2)
    yy = lax.div(ex, 4)
    dev = z * 8 + ex
    bdev, d = x_ref.shape
    f = w1_hbm.shape[2]
    half = d // 2
    H0, H1 = pl.ds(0, half), pl.ds(half, half)
    ALL = pl.ds(0, d)
    core = (z, ex + 1 - 2 * c)
    xn = (z, ex + 2 - 4 * xx)
    yn = (z, ex + 4 - 8 * yy)
    zp = {1: (z + 1 - 2 * lax.rem(z, 2), ex), 2: (z + 2 - 4 * lax.div(z, 2), ex), 3: (3 - z, ex)}

    def rows(k, dc, dq, n=1):
        return pl.ds(((k * 2 + dc) * 4 + dq) * bdev, n * bdev)

    SC0 = jax.named_scope
    barrier = pltpu.get_barrier_semaphore()

    def g0():
        for n in (core, xn, yn, zp[1], zp[2], zp[3]):
            pl.semaphore_signal(barrier, inc=1, device_id=n, device_id_type=MESH)
        _gates(idx_ref, gate_ref, GW.at[rows(0, 0, 0), :], IDX, GT)

    class send:
        def __init__(self, *args):
            self.args = args
            self.make().start()

        def make(self):
            src, dst, ss, rs, to = self.args
            return pltpu.make_async_remote_copy(src_ref=src(), dst_ref=dst(), send_sem=ss(), recv_sem=rs(),
                                                device_id=to, device_id_type=MESH)

        def wait_recv(self):
            self.make().wait_recv()

        def wait_send(self):
            self.make().wait_send()

    sent = []

    def flush():
        for cp in sent:
            cp.wait_send()
        sent.clear()

    ag = {}

    def ag_send(key, i, src_rows, dst_rows, cols, to):
        cp = send(lambda: U.at[src_rows, cols], lambda: U.at[dst_rows, cols], lambda: ag_s.at[i], lambda: ag_r.at[i], to)
        ag[key] = cp
        sent.append(cp)

    gw = {}

    def gw_send(key, i, src_rows, dst_rows, to):
        cp = send(lambda: GW.at[src_rows, :], lambda: GW.at[dst_rows, :], lambda: gw_s.at[i], lambda: gw_r.at[i], to)
        gw[key] = cp
        sent.append(cp)

    def a2(k, hh):
        cs = (H0, H1)[hh]
        near, far = (xn, yn) if hh == 0 else (yn, xn)
        nd, fd = (1, 2) if hh == 0 else (2, 1)
        ag_send(("2", k, hh), 6 + k * 8 + hh, rows(k, 0, 0), rows(k, 0, nd), cs, near)
        ag_send(("3", k, hh), 8 + k * 8 + hh, rows(k, 0, 0), rows(k, 0, fd), cs, far)

    def g1():
        with SC0("barrier"):
            pl.semaphore_wait(barrier, 6)
        for k in (1, 2, 3):
            gw_send(("z", k), k - 1, rows(0, 0, 0), rows(k, 0, 0), zp[k])

    def g2():
        for k in range(4):
            if k:
                gw[("z", k)].wait_recv()
            gw_send(("2", k), 3 + k * 3, rows(k, 0, 0), rows(k, 0, 1), xn)

    def g3():
        for k in range(4):
            gw[("2", k)].wait_recv()
            gw_send(("3", k), 4 + k * 3, rows(k, 0, 0, 2), rows(k, 0, 2, 2), yn)

    def g4():
        for k in range(4):
            gw[("3", k)].wait_recv()
            gw_send(("4", k), 5 + k * 3, rows(k, 0, 0, 4), rows(k, 1, 0, 4), core)

    def a3(k):
        ag[("2", k, 0)].wait_recv()
        ag_send(("4", k, 0), 10 + k * 8, rows(k, 0, 1), rows(k, 0, 3), H0, yn)
        ag[("2", k, 1)].wait_recv()
        ag_send(("4", k, 1), 11 + k * 8, rows(k, 0, 2), rows(k, 0, 3), H1, xn)

    def a4(k):
        for hh in range(2):
            ag[("3", k, hh)].wait_recv()
        ag_send(("5", k), 12 + k * 8, rows(k, 0, 0, 3), rows(k, 1, 0, 3), ALL, core)
        for hh in range(2):
            ag[("4", k, hh)].wait_recv()
        ag_send(("6", k), 13 + k * 8, rows(k, 0, 3), rows(k, 1, 3), ALL, core)

    def a5(k):
        ag[("5", k)].wait_recv()
        ag[("6", k)].wait_recv()

    def zwait(k):
        for hh in range(2):
            ag[("z", k, hh)].wait_recv()
            a2(k, hh)

    nh, l4 = wq_hbm.shape[1] // LANES, k_hbm.shape[1]
    pl.run_scoped(
        functools.partial(_attend, lens_ref, x_ref, ln1_ref, ln2_ref, k_hbm, v_hbm, wq_hbm, wo_hbm, h_ref,
                          U.at[rows(0, 0, 0), :], (g0, g1, g2)),
        pltpu.VMEM(wq_hbm.shape, BF16),
        pltpu.VMEM(wo_hbm.shape, BF16),
        pltpu.VMEM(k_hbm.shape, BF16),
        pltpu.VMEM(k_hbm.shape, BF16),
        pltpu.VMEM((nh * bdev, LANES), F32),
        pltpu.VMEM((nh * bdev, LANES), F32),
        pltpu.VMEM((bdev, d), BF16),
        pltpu.VMEM((bdev, nh * LANES), F32),
        pltpu.VMEM((l4, LANES), jnp.int32),
        pltpu.SemaphoreType.DMA((8,)),
        pltpu.SemaphoreType.DMA((8,)),
        pltpu.SemaphoreType.DMA((4,)),
        pltpu.SemaphoreType.DMA((4,)),
    )

    def experts(GB, Pb, G, W13, W2, S2, wsem, w2sem, s2sem):
        with SC0("ag_start"):
            for k in (1, 2, 3):
                for hh in range(2):
                    ag_send(("z", k, hh), (k - 1) * 2 + hh, rows(0, 0, 0), rows(k, 0, 0), (H0, H1)[hh], zp[k])
            a2(0, 0)
            a2(0, 1)
            g3()
        nt = f // 128
        L0, L1 = pl.ds(0, LANES), pl.ds(LANES, LANES)

        def load(src, dst, sem):
            pltpu.make_async_copy(src, dst, sem).start()

        def load13(a, b, e, base, count):
            def step(t):
                col = _at(t, LANES)
                load(a.at[e, :, col], W13.at[base + t, :, L0], wsem.at[base + t])
                load(b.at[e, :, col], W13.at[base + t, :, L1], wsem.at[base + t])
            _loop(count, step)

        load13(w1_hbm, w3_hbm, 0, 0, nt)
        load13(w1_hbm, w3_hbm, 1, nt, nt)
        sbase = lax.rem(dev, SHARED_DEVS) * 2
        for t in range(2):
            col = _at(sbase + t, LANES)
            load(s1_hbm.at[:, col], W13.at[2 * nt + t, :, L0], wsem.at[2 * nt + t])
            load(s3_hbm.at[:, col], W13.at[2 * nt + t, :, L1], wsem.at[2 * nt + t])
        scol = _at(sbase // 2, TILE)

        def load2(t):
            col = _at(t, TILE)
            for e in range(2):
                load(w2_hbm.at[e, :, col], W2.at[t, e], w2sem.at[t])
            load(s2_hbm.at[scol, col], S2.at[t], s2sem.at[t])
        _loop(d // TILE, load2)

        def got(ref, sem):
            pltpu.make_async_copy(ref, ref, sem).wait()

        with SC0("ag_z1"):
            zwait(1)
        with SC0("ag_30"):
            a3(0)
        with SC0("ag_z2"):
            zwait(2)
        with SC0("ag_31"):
            a3(1)
        with SC0("ag_z3"):
            zwait(3)
        with SC0("ag_41"):
            a4(1)
        with SC0("ag_32"):
            a3(2)
        g4()

        rs = {}

        def rs_send(key, i, src, dst, to):
            cp = send(src, dst, lambda: rs_s.at[i], lambda: rs_r.at[i], to)
            rs[key] = cp
            sent.append(cp)

        COLS = (H0, H1)

        def s1(k, hh):
            cs = COLS[hh]
            rs_send(("1", k, hh), k * 10 + hh, lambda: Pb.at[rows(k, 1, 0, 4), cs], lambda: R1.at[pl.ds(k * 64, 64), cs], core)

        def s2(k, hh):
            cs = COLS[hh]
            rs[("1", k, hh)].wait_recv()
            Pb[rows(k, 0, 0, 4), cs] = Pb[rows(k, 0, 0, 4), cs] + R1[pl.ds(k * 64, 64), cs]
            if hh == 0:
                rs_send(("2y", k), k * 10 + 2, lambda: Pb.at[rows(k, 0, 2, 2), H0], lambda: R2y.at[pl.ds(k * 32, 32), :], yn)
            else:
                rs_send(("2d", k), k * 10 + 3, lambda: Pb.at[rows(k, 0, 3), H1], lambda: R2x.at[pl.ds(k * 32 + 16, 16), :], xn)
                rs_send(("2x", k), k * 10 + 4, lambda: Pb.at[rows(k, 0, 1), H1], lambda: R2x.at[pl.ds(k * 32, 16), :], xn)

        def s3(k, hh):
            if hh == 0:
                rs[("2y", k)].wait_recv()
                Pb[rows(k, 0, 1), H0] = Pb[rows(k, 0, 1), H0] + R2y[pl.ds(k * 32 + 16, 16), :]
                rs_send(("3x", k), k * 10 + 5, lambda: Pb.at[rows(k, 0, 1), H0], lambda: R3x.at[pl.ds(k * 16, 16), :], xn)
                Pb[rows(k, 0, 0), H0] = Pb[rows(k, 0, 0), H0] + R2y[pl.ds(k * 32, 16), :]
            else:
                rs[("2d", k)].wait_recv()
                Pb[rows(k, 0, 2), H1] = Pb[rows(k, 0, 2), H1] + R2x[pl.ds(k * 32 + 16, 16), :]
                rs_send(("3y", k), k * 10 + 6, lambda: Pb.at[rows(k, 0, 2), H1], lambda: R3y.at[pl.ds(k * 16, 16), :], yn)
                rs[("2x", k)].wait_recv()
                Pb[rows(k, 0, 0), H1] = Pb[rows(k, 0, 0), H1] + R2x[pl.ds(k * 32, 16), :]

        def s4(k, hh):
            cs = COLS[hh]
            part = R3x if hh == 0 else R3y
            rs[("3x" if hh == 0 else "3y", k)].wait_recv()
            Pb[rows(k, 0, 0), cs] = Pb[rows(k, 0, 0), cs] + part[pl.ds(k * 16, 16), :]
            if k:
                rs_send(("4", k, hh), k * 10 + 7 + hh, lambda: Pb.at[rows(k, 0, 0), cs], lambda: R4.at[pl.ds(k * 16, 16), cs], zp[k])

        SC = jax.named_scope
        def chunk(ci, k0, n, first, hooks):
            m = n * 8 * bdev
            cr = pl.ds(k0 * 8 * bdev, m)
            mr = pl.ds(0, m)
            lanes = lax.broadcasted_iota(jnp.int32, (m, LANES), 1)
            steps = (2 * nt + 2) // UNROLL
            last = ci == len(CHUNKS) - 1
            un2 = UNROLL2 // 2 if last else UNROLL2

            def hook(i):
                if hooks.get(i):
                    with SC(f"c{ci}_hook{i}"):
                        for fn, *a in hooks[i]:
                            fn(*a)

            def up(t):
                zz = jnp.dot(U[cr, :], W13[t], preferred_element_type=F32)
                z1, z3 = zz[:, :128], zz[:, 128:]
                g = z1 * jax.nn.sigmoid(z1) * z3
                g = jnp.where((t < 2 * nt) | (dev < SHARED_DEVS), g, 0.0)
                G[mr, _at(t, LANES)] = g.astype(BF16)

            def ups(t):
                if first:
                    for v in range(UNROLL):
                        got(W13.at[t * UNROLL + v], wsem.at[t * UNROLL + v])
                for v in range(UNROLL):
                    up(t * UNROLL + v)
                for p in range(steps - 1):
                    if hooks.get(p):
                        @pl.when(t == p)
                        def _(p=p):
                            hook(p)

            def down(t):
                acc = jnp.dot(G[mr, pl.ds(2 * f, 256)], S2[t], preferred_element_type=F32)
                for e in range(2):
                    r = jnp.dot(G[mr, pl.ds(e * f, f)], W2[t, e], preferred_element_type=F32).astype(BF16).astype(F32)
                    g = GB[e, mr, :]
                    g = jnp.concatenate([g, g], axis=1)
                    acc = acc + jnp.where(g > 0, g * r, 0.0)
                Pb[cr, _at(t, TILE)] = acc

            def downs(t):
                if first:
                    for v in range(un2):
                        got(W2.at[t * un2 + v], w2sem.at[t * un2 + v])
                        got(S2.at[t * un2 + v], s2sem.at[t * un2 + v])
                for v in range(un2):
                    down(t * un2 + v)

                if hooks.get(3) and last:
                    @pl.when(t == 0)
                    def _():
                        hook(3)

            with SC(f"c{ci}_gates"):
                for e in range(2):
                    gv = jnp.sum(jnp.where(lanes == dev * 2 + e, GW[cr, :], 0.0), axis=1, keepdims=True)
                    GB[e, mr, :] = jnp.broadcast_to(gv, (m, LANES))
            with SC(f"c{ci}_up"):
                _loop(steps, ups)
            if last:
                flush()
            hook(2)
            with SC(f"c{ci}_down"):
                _loop(d // TILE // un2, downs)
            if not last:
                hook(3)
            hook(4)

        for ci, (k0, n) in enumerate(CHUNKS):
            for k in range(k0, k0 + n):
                with SC(f"c{ci}_a5"):
                    a5(k)
                    gw[("4", k)].wait_recv()
            chunk(ci, k0, n, ci == 0, HOOKS(ci, a2, zwait, a3, a4, a5, s1, s2, s3, s4))
        ka, kb = CHUNKS[-2][0], CHUNKS[-1][0]
        with SC("t_s2"):
            s2(kb, 0)
            s2(kb, 1)
        with SC("t_s4a"):
            s4(ka, 0)
            s4(ka, 1)
        with SC("t_s3"):
            s3(kb, 0)
            s3(kb, 1)
        with SC("t_s4"):
            s4(kb, 0)
            s4(kb, 1)

        acc = h_ref[...].astype(F32) + Pb[rows(0, 0, 0), :]
        for k in (1, 2, 3):
            with SC(f"t_s5{k}"):
                rs[("4", k, 0)].wait_recv()
                rs[("4", k, 1)].wait_recv()
            acc = acc + R4[pl.ds(k * 16, 16), :]
        y_ref[...] = acc.astype(BF16)
        flush()

    mmax = max(n for _, n in CHUNKS) * 8 * bdev
    f = w1_hbm.shape[2]
    pl.run_scoped(
        experts,
        pltpu.VMEM((2, mmax, LANES), F32),
        pltpu.VMEM((bdev * 32, d), F32),
        pltpu.VMEM((mmax, 2 * f + TILE), BF16),
        pltpu.VMEM((2 * f // LANES + 2, d, TILE), BF16),
        pltpu.VMEM((d // TILE, 2, f, TILE), BF16),
        pltpu.VMEM((d // TILE, TILE, TILE), BF16),
        pltpu.SemaphoreType.DMA((2 * f // LANES + 2,)),
        pltpu.SemaphoreType.DMA((d // TILE,)),
        pltpu.SemaphoreType.DMA((d // TILE,)),
    )


def solution(mesh):
    def body(x, kv_k, kv_v, lens, idx, gates, ln1, wq, wo, ln2, ws1, ws3, ws2, w1, w3, w2):
        bdev, d = x.shape
        _, l, kvh, hd = kv_k.shape
        rows = bdev * 32
        vm = pl.BlockSpec(memory_space=pltpu.VMEM)
        hbm = pl.BlockSpec(memory_space=pl.ANY)
        kv = (bdev, l * kvh, hd)
        sem = pltpu.SemaphoreType.DMA
        return pl.pallas_call(
            _layer_kernel,
            out_shape=jax.ShapeDtypeStruct((bdev, d), BF16),
            in_specs=[pl.BlockSpec(memory_space=pltpu.SMEM)] + [vm] * 5 + [hbm] * 10,
            out_specs=vm,
            scratch_shapes=[
                pltpu.VMEM((bdev, d), BF16),
                pltpu.VMEM((8, LANES), jnp.int32),
                pltpu.VMEM((8, LANES), F32),
                pltpu.VMEM((rows, d), BF16),
                pltpu.VMEM((rows, LANES), F32),
                pltpu.VMEM((rows // 2, d), F32),
                pltpu.VMEM((rows // 4, d // 2), F32),
                pltpu.VMEM((rows // 4, d // 2), F32),
                pltpu.VMEM((rows // 8, d // 2), F32),
                pltpu.VMEM((rows // 8, d // 2), F32),
                pltpu.VMEM((rows // 8, d), F32),
                sem((38,)), sem((38,)), sem((16,)), sem((16,)), sem((40,)), sem((40,)),
            ],
            compiler_params=pltpu.CompilerParams(
                collective_id=0, has_side_effects=True, vmem_limit_bytes=62 * 1024 * 1024
            ),
        )(lens, x, ln1.reshape(d // LANES, LANES), ln2.reshape(d // LANES, LANES), idx.T, gates.T,
          kv_k.reshape(kv), kv_v.reshape(kv), wq, wo, ws1, ws3, ws2, w1, w3, w2)

    rows = P(GRP)
    rep = P()
    return jax.shard_map(
        body, mesh=mesh,
        in_specs=(rows, rows, rows, rows, rows, rows, rep, rep, rep, rep, rep, rep, rep, rows, rows, rows),
        out_specs=rows, check_vma=False)
```

```python
import functools

import jax
import jax.numpy as jnp
from jax import lax
from jax.experimental import pallas as pl
from jax.experimental.pallas import tpu as pltpu
from jax.sharding import PartitionSpec as P

EPS = 1e-6
GRP = ("ey", "ex")
MESH = pl.DeviceIdType.MESH
BF16, F32 = jnp.bfloat16, jnp.float32

LANES, TILE = 128, 256


def _loop(n, step):
    def body(t, carry):
        step(t)
        return carry
    lax.fori_loop(0, n, body, 0)


def _at(t, width):
    return pl.ds(pl.multiple_of(t * width, width), width)


SHARED_DEVS = 22
CHUNKS = ((1, 1), (2, 1), (3, 1), (0, 1))
UNROLL, UNROLL2, PAIR = 12, 8, 1


def HOOKS(ci, a2, zwait, a3, a4, a5, s1, s2, s3, s4):
    order = [k for k, _ in CHUNKS]
    k = order[ci]
    ev = {i: [] for i in range(5)}
    if ci == 0:
        ev[0] += [(a3, 3), (a4, 2)]
        ev[2] += [(a4, 0)]
        ev[4] += [(a4, 3)]
    if ci >= 2:
        ev[2] += [(s4, order[ci - 2], 0), (s4, order[ci - 2], 1)]
    if ci >= 1:
        ev[0] += [(s2, order[ci - 1], 0), (s2, order[ci - 1], 1)]
    ev[3] += [(s1, k, 0)]
    ev[4] += [(s1, k, 1)]
    if ci >= 1:
        ev[4] += [(s3, order[ci - 1], 0), (s3, order[ci - 1], 1)]
    return ev


def _norm(v, ln_ref):
    r = lax.rsqrt(jnp.mean(v * v, axis=-1, keepdims=True) + EPS)
    n = v.shape[1] // 128
    return jnp.concatenate(
        [(v[:, i * 128:(i + 1) * 128] * r * ln_ref[i:i + 1, :].astype(F32)).astype(BF16) for i in range(n)], axis=1)


def _attend(lens_ref, x_ref, ln1_ref, ln2_ref, k_hbm, v_hbm, wq_hbm, wo_hbm, h_ref, u_ref, between,
            WQ, WO, K, V, QS, OS, A, ACC, POS, qsem, osem, ksem, vsem):
    b, d = x_ref.shape
    hd = LANES
    nh = wq_hbm.shape[1] // hd
    rows = K.shape[1]
    kvh = rows // 256
    grp = nh // kvh
    nq, no, nk = qsem.shape[0], osem.shape[0], ksem.shape[0]
    cq, co, ck = d // nq, (nh * hd) // no, b // nk

    def cpq(i):
        return pltpu.make_async_copy(wq_hbm.at[_at(i, cq), :], WQ.at[_at(i, cq), :], qsem.at[i])

    def cpo(i):
        return pltpu.make_async_copy(wo_hbm.at[_at(i, co), :], WO.at[_at(i, co), :], osem.at[i])

    def cpk(i):
        return pltpu.make_async_copy(k_hbm.at[pl.ds(i * ck, ck)], K.at[pl.ds(i * ck, ck)], ksem.at[i])

    def cpv(i):
        return pltpu.make_async_copy(v_hbm.at[pl.ds(i * ck, ck)], V.at[pl.ds(i * ck, ck)], vsem.at[i])

    _loop(nq, lambda i: cpq(i).start())
    xf = x_ref[...].astype(F32)
    A[...] = _norm(xf, ln1_ref)
    ACC[...] = jnp.zeros(ACC.shape, F32)
    row = lax.broadcasted_iota(jnp.int32, (rows, LANES), 0)
    lane = lax.broadcasted_iota(jnp.int32, (rows, LANES), 1)
    own = lax.rem(row, kvh) == lax.div(lax.rem(lane, nh), grp)
    POS[...] = jnp.where(own, lax.div(row, kvh), 1 << 20)
    between[0]()

    def queries(i):
        cpq(i).wait()

        @pl.when(i >= nq - nk)
        def _():
            cpk(i - (nq - nk)).start()
            cpv(i - (nq - nk)).start()
        ACC[...] = ACC[...] + jnp.dot(A[:, _at(i, cq)], WQ[_at(i, cq), :], preferred_element_type=F32)
    _loop(nq, queries)
    _loop(no, lambda i: cpo(i).start())
    for i in range(nh):
        QS[i * b:(i + 1) * b, :] = ACC[:, i * hd:(i + 1) * hd].astype(BF16).astype(F32)
    between[1]()

    lane1 = lax.div(lax.broadcasted_iota(jnp.int32, (1, LANES), 1), nh)
    slot = lax.div(lax.broadcasted_iota(jnp.int32, (LANES, LANES), 1), nh)
    scale = hd ** -0.5 * 1.4426950408889634

    def group(g):
        first = g * ck
        q = jnp.concatenate([QS[pl.ds(first + i, nh, stride=b), :] for i in range(ck)], axis=0)
        qt = jnp.transpose(q)
        qq = jnp.concatenate([jnp.where(slot == i, qt, 0.0).astype(BF16) for i in range(ck)], axis=0)
        kc = jnp.concatenate([K[first + i] for i in range(ck)], axis=1)
        s = jnp.dot(kc, qq, preferred_element_type=F32)
        n = jnp.zeros(lane1.shape, jnp.int32)
        for i in range(ck):
            n = jnp.where(lane1 == i, lens_ref[first + i], n)
        s = jnp.where(POS[...] < n, s, -jnp.inf)
        p = jnp.exp2((s - jnp.max(s, axis=0, keepdims=True)) * scale)
        p = (p * (1.0 / jnp.sum(p, axis=0, keepdims=True))).astype(BF16)
        pt = jnp.transpose(p)
        for i in range(ck):
            o = jnp.dot(pt[i * nh:(i + 1) * nh, :], V[first + i], preferred_element_type=F32)
            OS[pl.ds(first + i, nh, stride=b), :] = o.astype(BF16).astype(F32)
    def groups(t):
        for g in range(PAIR):
            cpk(t * PAIR + g).wait()
            cpv(t * PAIR + g).wait()
        for g in range(PAIR):
            group(t * PAIR + g)
    _loop(nk // PAIR, groups)
    between[2]()

    ACC[:, 0:d] = jnp.zeros((b, d), F32)

    def outs(i):
        cpo(i).wait()
        n = co // hd
        o = jnp.concatenate([OS[pl.ds(pl.multiple_of((i * n + j) * b, b), b), :].astype(BF16) for j in range(n)], axis=1)
        ACC[:, 0:d] = ACC[:, 0:d] + jnp.dot(o, WO[_at(i, co), :], preferred_element_type=F32)
    _loop(no, outs)
    h = (xf + ACC[:, 0:d]).astype(BF16)
    h_ref[...] = h
    u_ref[...] = _norm(h.astype(F32), ln2_ref)


def _gates(idx_ref, gate_ref, gw_ref, IDX, GT):
    top, b = idx_ref.shape
    cap = b - b // 8
    IDX[...] = jnp.zeros(IDX.shape, jnp.int32)
    GT[...] = jnp.zeros(GT.shape, F32)
    IDX[0:top, 0:b] = idx_ref[...]
    GT[0:top, 0:b] = gate_ref[...]
    expert = lax.broadcasted_iota(jnp.int32, (LANES, LANES), 0)
    oh = jnp.zeros((LANES, LANES), F32)
    gm = jnp.zeros((LANES, LANES), F32)
    for j in range(top):
        hit = IDX[j:j + 1, :] == expert
        oh = oh + jnp.where(hit, 1.0, 0.0)
        gm = gm + jnp.where(hit, GT[j:j + 1, :], 0.0)
    before = jnp.where(expert < lax.broadcasted_iota(jnp.int32, (LANES, LANES), 1), 1.0, 0.0)
    rank = jnp.dot(oh.astype(BF16), before.astype(BF16), preferred_element_type=F32)
    gw_ref[...] = jnp.transpose(jnp.where(rank < cap - 0.5, gm, 0.0))[0:b, :]


def _layer_kernel(lens_ref, x_ref, ln1_ref, ln2_ref, idx_ref, gate_ref, k_hbm, v_hbm, wq_hbm, wo_hbm,
                  s1_hbm, s3_hbm, s2_hbm, w1_hbm, w3_hbm, w2_hbm, y_ref, h_ref, IDX, GT,
                  U, GW, R1, R2x, R2y, R3x, R3y, R4,
                  ag_s, ag_r, gw_s, gw_r, rs_s, rs_r):
    z = lax.axis_index("ey")
    ex = lax.axis_index("ex")
    c = lax.rem(ex, 2)
    xx = lax.rem(lax.div(ex, 2), 2)
    yy = lax.div(ex, 4)
    dev = z * 8 + ex
    bdev, d = x_ref.shape
    f = w1_hbm.shape[2]
    half = d // 2
    H0, H1 = pl.ds(0, half), pl.ds(half, half)
    ALL = pl.ds(0, d)
    core = (z, ex + 1 - 2 * c)
    xn = (z, ex + 2 - 4 * xx)
    yn = (z, ex + 4 - 8 * yy)
    zp = {1: (z + 1 - 2 * lax.rem(z, 2), ex), 2: (z + 2 - 4 * lax.div(z, 2), ex), 3: (3 - z, ex)}

    def rows(k, dc, dq, n=1):
        return pl.ds(((k * 2 + dc) * 4 + dq) * bdev, n * bdev)

    SC0 = jax.named_scope
    barrier = pltpu.get_barrier_semaphore()

    def g0():
        for n in (core, xn, yn, zp[1], zp[2], zp[3]):
            pl.semaphore_signal(barrier, inc=1, device_id=n, device_id_type=MESH)
        _gates(idx_ref, gate_ref, GW.at[rows(0, 0, 0), :], IDX, GT)

    class send:
        def __init__(self, *args):
            self.args = args
            self.make().start()

        def make(self):
            src, dst, ss, rs, to = self.args
            return pltpu.make_async_remote_copy(src_ref=src(), dst_ref=dst(), send_sem=ss(), recv_sem=rs(),
                                                device_id=to, device_id_type=MESH)

        def wait_recv(self):
            self.make().wait_recv()

        def wait_send(self):
            self.make().wait_send()

    sent = []

    def flush():
        for cp in sent:
            cp.wait_send()
        sent.clear()

    ag = {}

    def ag_send(key, i, src_rows, dst_rows, cols, to):
        cp = send(lambda: U.at[src_rows, cols], lambda: U.at[dst_rows, cols], lambda: ag_s.at[i], lambda: ag_r.at[i], to)
        ag[key] = cp
        sent.append(cp)

    gw = {}

    def gw_send(key, i, src_rows, dst_rows, to):
        cp = send(lambda: GW.at[src_rows, :], lambda: GW.at[dst_rows, :], lambda: gw_s.at[i], lambda: gw_r.at[i], to)
        gw[key] = cp
        sent.append(cp)

    def a2(k, hh):
        cs = (H0, H1)[hh]
        near, far = (xn, yn) if hh == 0 else (yn, xn)
        nd, fd = (1, 2) if hh == 0 else (2, 1)
        ag_send(("2", k, hh), 6 + k * 8 + hh, rows(k, 0, 0), rows(k, 0, nd), cs, near)
        ag_send(("3", k, hh), 8 + k * 8 + hh, rows(k, 0, 0), rows(k, 0, fd), cs, far)

    def g1():
        with SC0("barrier"):
            pl.semaphore_wait(barrier, 6)
        for k in (1, 2, 3):
            gw_send(("z", k), k - 1, rows(0, 0, 0), rows(k, 0, 0), zp[k])

    def g2():
        for k in range(4):
            if k:
                gw[("z", k)].wait_recv()
            gw_send(("2", k), 3 + k * 3, rows(k, 0, 0), rows(k, 0, 1), xn)

    def g3():
        for k in range(4):
            gw[("2", k)].wait_recv()
            gw_send(("3", k), 4 + k * 3, rows(k, 0, 0, 2), rows(k, 0, 2, 2), yn)

    def g4():
        for k in range(4):
            gw[("3", k)].wait_recv()
            gw_send(("4", k), 5 + k * 3, rows(k, 0, 0, 4), rows(k, 1, 0, 4), core)

    def a3(k):
        ag[("2", k, 0)].wait_recv()
        ag_send(("4", k, 0), 10 + k * 8, rows(k, 0, 1), rows(k, 0, 3), H0, yn)
        ag[("2", k, 1)].wait_recv()
        ag_send(("4", k, 1), 11 + k * 8, rows(k, 0, 2), rows(k, 0, 3), H1, xn)

    def a4(k):
        for hh in range(2):
            ag[("3", k, hh)].wait_recv()
        ag_send(("5", k), 12 + k * 8, rows(k, 0, 0, 3), rows(k, 1, 0, 3), ALL, core)
        for hh in range(2):
            ag[("4", k, hh)].wait_recv()
        ag_send(("6", k), 13 + k * 8, rows(k, 0, 3), rows(k, 1, 3), ALL, core)

    def a5(k):
        ag[("5", k)].wait_recv()
        ag[("6", k)].wait_recv()

    def zwait(k):
        for hh in range(2):
            ag[("z", k, hh)].wait_recv()
            a2(k, hh)

    nh, l4 = wq_hbm.shape[1] // LANES, k_hbm.shape[1]
    pl.run_scoped(
        functools.partial(_attend, lens_ref, x_ref, ln1_ref, ln2_ref, k_hbm, v_hbm, wq_hbm, wo_hbm, h_ref,
                          U.at[rows(0, 0, 0), :], (g0, g1, g2)),
        pltpu.VMEM(wq_hbm.shape, BF16),
        pltpu.VMEM(wo_hbm.shape, BF16),
        pltpu.VMEM(k_hbm.shape, BF16),
        pltpu.VMEM(k_hbm.shape, BF16),
        pltpu.VMEM((nh * bdev, LANES), F32),
        pltpu.VMEM((nh * bdev, LANES), F32),
        pltpu.VMEM((bdev, d), BF16),
        pltpu.VMEM((bdev, nh * LANES), F32),
        pltpu.VMEM((l4, LANES), jnp.int32),
        pltpu.SemaphoreType.DMA((8,)),
        pltpu.SemaphoreType.DMA((8,)),
        pltpu.SemaphoreType.DMA((4,)),
        pltpu.SemaphoreType.DMA((4,)),
    )

    def experts(GB, Pb, G, W13, W2, S2, wsem, w2sem, s2sem):
        with SC0("ag_start"):
            for k in (1, 2, 3):
                for hh in range(2):
                    ag_send(("z", k, hh), (k - 1) * 2 + hh, rows(0, 0, 0), rows(k, 0, 0), (H0, H1)[hh], zp[k])
            a2(0, 0)
            a2(0, 1)
            g3()
        nt = f // 128
        L0, L1 = pl.ds(0, LANES), pl.ds(LANES, LANES)

        def load(src, dst, sem):
            pltpu.make_async_copy(src, dst, sem).start()

        def load13(a, b, e, base, count):
            def step(t):
                col = _at(t, LANES)
                load(a.at[e, :, col], W13.at[base + t, :, L0], wsem.at[base + t])
                load(b.at[e, :, col], W13.at[base + t, :, L1], wsem.at[base + t])
            _loop(count, step)

        load13(w1_hbm, w3_hbm, 0, 0, nt)
        load13(w1_hbm, w3_hbm, 1, nt, nt)
        sbase = lax.rem(dev, SHARED_DEVS) * 2
        for t in range(2):
            col = _at(sbase + t, LANES)
            load(s1_hbm.at[:, col], W13.at[2 * nt + t, :, L0], wsem.at[2 * nt + t])
            load(s3_hbm.at[:, col], W13.at[2 * nt + t, :, L1], wsem.at[2 * nt + t])
        scol = _at(sbase // 2, TILE)

        def load2(t):
            col = _at(t, TILE)
            for e in range(2):
                load(w2_hbm.at[e, :, col], W2.at[t, e], w2sem.at[t])
            load(s2_hbm.at[scol, col], S2.at[t], s2sem.at[t])
        _loop(d // TILE, load2)

        def got(ref, sem):
            pltpu.make_async_copy(ref, ref, sem).wait()

        with SC0("ag_z1"):
            zwait(1)
        with SC0("ag_30"):
            a3(0)
        with SC0("ag_z2"):
            zwait(2)
        with SC0("ag_31"):
            a3(1)
        with SC0("ag_z3"):
            zwait(3)
        with SC0("ag_41"):
            a4(1)
        with SC0("ag_32"):
            a3(2)
        g4()

        rs = {}

        def rs_send(key, i, src, dst, to):
            cp = send(src, dst, lambda: rs_s.at[i], lambda: rs_r.at[i], to)
            rs[key] = cp
            sent.append(cp)

        COLS = (H0, H1)

        def s1(k, hh):
            cs = COLS[hh]
            rs_send(("1", k, hh), k * 10 + hh, lambda: Pb.at[rows(k, 1, 0, 4), cs], lambda: R1.at[pl.ds(k * 64, 64), cs], core)

        def s2(k, hh):
            cs = COLS[hh]
            rs[("1", k, hh)].wait_recv()
            Pb[rows(k, 0, 0, 4), cs] = Pb[rows(k, 0, 0, 4), cs] + R1[pl.ds(k * 64, 64), cs]
            if hh == 0:
                rs_send(("2y", k), k * 10 + 2, lambda: Pb.at[rows(k, 0, 2, 2), H0], lambda: R2y.at[pl.ds(k * 32, 32), :], yn)
            else:
                rs_send(("2d", k), k * 10 + 3, lambda: Pb.at[rows(k, 0, 3), H1], lambda: R2x.at[pl.ds(k * 32 + 16, 16), :], xn)
                rs_send(("2x", k), k * 10 + 4, lambda: Pb.at[rows(k, 0, 1), H1], lambda: R2x.at[pl.ds(k * 32, 16), :], xn)

        def s3(k, hh):
            if hh == 0:
                rs[("2y", k)].wait_recv()
                Pb[rows(k, 0, 1), H0] = Pb[rows(k, 0, 1), H0] + R2y[pl.ds(k * 32 + 16, 16), :]
                rs_send(("3x", k), k * 10 + 5, lambda: Pb.at[rows(k, 0, 1), H0], lambda: R3x.at[pl.ds(k * 16, 16), :], xn)
                Pb[rows(k, 0, 0), H0] = Pb[rows(k, 0, 0), H0] + R2y[pl.ds(k * 32, 16), :]
            else:
                rs[("2d", k)].wait_recv()
                Pb[rows(k, 0, 2), H1] = Pb[rows(k, 0, 2), H1] + R2x[pl.ds(k * 32 + 16, 16), :]
                rs_send(("3y", k), k * 10 + 6, lambda: Pb.at[rows(k, 0, 2), H1], lambda: R3y.at[pl.ds(k * 16, 16), :], yn)
                rs[("2x", k)].wait_recv()
                Pb[rows(k, 0, 0), H1] = Pb[rows(k, 0, 0), H1] + R2x[pl.ds(k * 32, 16), :]

        def s4(k, hh):
            cs = COLS[hh]
            part = R3x if hh == 0 else R3y
            rs[("3x" if hh == 0 else "3y", k)].wait_recv()
            Pb[rows(k, 0, 0), cs] = Pb[rows(k, 0, 0), cs] + part[pl.ds(k * 16, 16), :]
            if k:
                rs_send(("4", k, hh), k * 10 + 7 + hh, lambda: Pb.at[rows(k, 0, 0), cs], lambda: R4.at[pl.ds(k * 16, 16), cs], zp[k])

        SC = jax.named_scope
        def chunk(ci, k0, n, first, hooks):
            m = n * 8 * bdev
            cr = pl.ds(k0 * 8 * bdev, m)
            mr = pl.ds(0, m)
            lanes = lax.broadcasted_iota(jnp.int32, (m, LANES), 1)
            steps = (2 * nt + 2) // UNROLL
            last = ci == len(CHUNKS) - 1
            un2 = UNROLL2 // 2 if last else UNROLL2

            def hook(i):
                if hooks.get(i):
                    with SC(f"c{ci}_hook{i}"):
                        for fn, *a in hooks[i]:
                            fn(*a)

            def up(t):
                zz = jnp.dot(U[cr, :], W13[t], preferred_element_type=F32)
                z1, z3 = zz[:, :128], zz[:, 128:]
                g = z1 * jax.nn.sigmoid(z1) * z3
                g = jnp.where((t < 2 * nt) | (dev < SHARED_DEVS), g, 0.0)
                G[mr, _at(t, LANES)] = g.astype(BF16)

            def ups(t):
                if first:
                    for v in range(UNROLL):
                        got(W13.at[t * UNROLL + v], wsem.at[t * UNROLL + v])
                for v in range(UNROLL):
                    up(t * UNROLL + v)
                for p in range(steps - 1):
                    if hooks.get(p):
                        @pl.when(t == p)
                        def _(p=p):
                            hook(p)

            def down(t):
                acc = jnp.dot(G[mr, pl.ds(2 * f, 256)], S2[t], preferred_element_type=F32)
                for e in range(2):
                    r = jnp.dot(G[mr, pl.ds(e * f, f)], W2[t, e], preferred_element_type=F32).astype(BF16).astype(F32)
                    g = GB[e, mr, :]
                    g = jnp.concatenate([g, g], axis=1)
                    acc = acc + jnp.where(g > 0, g * r, 0.0)
                Pb[cr, _at(t, TILE)] = acc

            def downs(t):
                if first:
                    for v in range(un2):
                        got(W2.at[t * un2 + v], w2sem.at[t * un2 + v])
                        got(S2.at[t * un2 + v], s2sem.at[t * un2 + v])
                for v in range(un2):
                    down(t * un2 + v)

                if hooks.get(3) and last:
                    @pl.when(t == 0)
                    def _():
                        hook(3)

            with SC(f"c{ci}_gates"):
                for e in range(2):
                    gv = jnp.sum(jnp.where(lanes == dev * 2 + e, GW[cr, :], 0.0), axis=1, keepdims=True)
                    GB[e, mr, :] = jnp.broadcast_to(gv, (m, LANES))
            with SC(f"c{ci}_up"):
                _loop(steps, ups)
            if last:
                flush()
            hook(2)
            with SC(f"c{ci}_down"):
                _loop(d // TILE // un2, downs)
            if not last:
                hook(3)
            hook(4)

        for ci, (k0, n) in enumerate(CHUNKS):
            for k in range(k0, k0 + n):
                with SC(f"c{ci}_a5"):
                    a5(k)
                    gw[("4", k)].wait_recv()
            chunk(ci, k0, n, ci == 0, HOOKS(ci, a2, zwait, a3, a4, a5, s1, s2, s3, s4))
        ka, kb = CHUNKS[-2][0], CHUNKS[-1][0]
        with SC("t_s2"):
            s2(kb, 0)
            s2(kb, 1)
        with SC("t_s4a"):
            s4(ka, 0)
            s4(ka, 1)
        with SC("t_s3"):
            s3(kb, 0)
            s3(kb, 1)
        with SC("t_s4"):
            s4(kb, 0)
            s4(kb, 1)

        acc = h_ref[...].astype(F32) + Pb[rows(0, 0, 0), :]
        for k in (1, 2, 3):
            with SC(f"t_s5{k}"):
                rs[("4", k, 0)].wait_recv()
                rs[("4", k, 1)].wait_recv()
            acc = acc + R4[pl.ds(k * 16, 16), :]
        y_ref[...] = acc.astype(BF16)
        flush()

    mmax = max(n for _, n in CHUNKS) * 8 * bdev
    f = w1_hbm.shape[2]
    pl.run_scoped(
        experts,
        pltpu.VMEM((2, mmax, LANES), F32),
        pltpu.VMEM((bdev * 32, d), F32),
        pltpu.VMEM((mmax, 2 * f + TILE), BF16),
        pltpu.VMEM((2 * f // LANES + 2, d, TILE), BF16),
        pltpu.VMEM((d // TILE, 2, f, TILE), BF16),
        pltpu.VMEM((d // TILE, TILE, TILE), BF16),
        pltpu.SemaphoreType.DMA((2 * f // LANES + 2,)),
        pltpu.SemaphoreType.DMA((d // TILE,)),
        pltpu.SemaphoreType.DMA((d // TILE,)),
    )


def solution(mesh):
    def body(x, kv_k, kv_v, lens, idx, gates, ln1, wq, wo, ln2, ws1, ws3, ws2, w1, w3, w2):
        bdev, d = x.shape
        _, l, kvh, hd = kv_k.shape
        rows = bdev * 32
        vm = pl.BlockSpec(memory_space=pltpu.VMEM)
        hbm = pl.BlockSpec(memory_space=pl.ANY)
        kv = (bdev, l * kvh, hd)
        sem = pltpu.SemaphoreType.DMA
        return pl.pallas_call(
            _layer_kernel,
            out_shape=jax.ShapeDtypeStruct((bdev, d), BF16),
            in_specs=[pl.BlockSpec(memory_space=pltpu.SMEM)] + [vm] * 5 + [hbm] * 10,
            out_specs=vm,
            scratch_shapes=[
                pltpu.VMEM((bdev, d), BF16),
                pltpu.VMEM((8, LANES), jnp.int32),
                pltpu.VMEM((8, LANES), F32),
                pltpu.VMEM((rows, d), BF16),
                pltpu.VMEM((rows, LANES), F32),
                pltpu.VMEM((rows // 2, d), F32),
                pltpu.VMEM((rows // 4, d // 2), F32),
                pltpu.VMEM((rows // 4, d // 2), F32),
                pltpu.VMEM((rows // 8, d // 2), F32),
                pltpu.VMEM((rows // 8, d // 2), F32),
                pltpu.VMEM((rows // 8, d), F32),
                sem((38,)), sem((38,)), sem((16,)), sem((16,)), sem((40,)), sem((40,)),
            ],
            compiler_params=pltpu.CompilerParams(
                collective_id=0, has_side_effects=True, vmem_limit_bytes=62 * 1024 * 1024
            ),
        )(lens, x, ln1.reshape(d // LANES, LANES), ln2.reshape(d // LANES, LANES), idx.T, gates.T,
          kv_k.reshape(kv), kv_v.reshape(kv), wq, wo, ws1, ws3, ws2, w1, w3, w2)

    rows = P(GRP)
    rep = P()
    return jax.shard_map(
        body, mesh=mesh,
        in_specs=(rows, rows, rows, rows, rows, rows, rep, rep, rep, rep, rep, rep, rep, rows, rows, rows),
        out_specs=rows, check_vma=False)
```
